128 devices in a mesh: gx: 8 (over z_hi, x), gy: 4 (over z_lo, core), gz: 4 (over y).
Axes of the slice: x: 4, y: 4, z: 4 (z_hi: 2, z_lo: 2; z = z_hi * 2 + z_lo), core: 2. Of those that a mesh axis runs over, the one named last changes fastest.
Arguments:
- calcium: float32 [8, 256, 128, 512], P(None, 'gx', 'gz', 'gy'), may hold values from 0.1 to 3
- activation: float32 [8, 256, 128, 512], P(None, 'gx', 'gz', 'gy'), may hold values from 0 to 1
- element_first: int32 [256], replicated, may hold values from 0 to 63, as said below
- offset_first: float32 [256], replicated, may hold values from 0.1 to 0.9
- element_second: int32 [512], replicated, may hold values from 0 to 127, as said below
- offset_second: float32 [512], replicated, may hold values from 0.1 to 0.9
- element_third: int32 [128], replicated, may hold values from 0 to 31, as said below
- offset_third: float32 [128], replicated, may hold values from 0.1 to 0.9
- troponin: float32 [64, 32, 128], P('gx', ('gy', 'gz')), may hold values from 0 to 1
- tension: float32 [64, 32, 128], P('gx', ('gy', 'gz')), may hold values from 0 to 2
- unbind_rate: float32 [64, 32, 128], P('gx', ('gy', 'gz')), may hold values from 0.2 to 2
- relax_rate: float32 [64, 32, 128], P('gx', ('gy', 'gz')), may hold values from 0.5 to 4
Outputs:
- bound_fraction: float32 [64, 32, 128], P('gx', ('gy', 'gz'))
- active_tension: float32 [64, 32, 128], P('gx', ('gy', 'gz'))
The draws below stay inside these ranges and needn't reach their ends.
Inputs may be any that keep to these rules, and one draw needn't show every extreme that they name: `element_first`: never falling; the cells of each aligned block of 32 cells belong to that block's own 8 elements, each element holding at least one cell. `element_second`: never falling; the cells of each aligned block of 128 cells belong to that block's own 32 elements, each element holding at least one cell. `element_third`: never falling; the cells of each aligned block of 8 cells belong to that block's own 2 elements, each element holding at least one cell.
All inputs are finite; a program needn't handle non-finite values.
Results may differ from the reference program's by a relative error of at most 0.00005.
Values sent between devices are 32-bit elements.
A program may use at most 64 MiB of HBM per device.

```python
import math
import jax
import jax.numpy as jnp
from jax import lax

EX_DEV = 8
EY_DEV = 32
EZ_BLK = 2
SUB = 8
FX_BLK = 32
FY_BLK = 128
FZ_BLK = 8
NXC = 64
NYC = 128
NZC = 32
NXF = 256
NYF = 512
NZF = 128


def block_elements(key, blocks, cells, elements):

    def single(block_key):
        scores = jax.random.permutation(block_key, cells - 1) + 1
        cut_points = jnp.sort(scores[:elements - 1])
        places = jnp.arange(cells)
        return jnp.sum((places[:, None] >= cut_points[None, :]).astype(jnp.int32), axis=1)
    block_keys = jax.random.split(key, blocks)
    within = jax.vmap(single)(block_keys)
    offsets = elements * jnp.arange(blocks)[:, None]
    return (within + offsets).reshape(-1).astype(jnp.int32)


def draw_element_first(key, part):
    return block_elements(jax.random.fold_in(key, 11), NXF // FX_BLK, FX_BLK, EX_DEV)


def draw_element_second(key, part):
    return block_elements(jax.random.fold_in(key, 23), NYF // FY_BLK, FY_BLK, EY_DEV)


def draw_element_third(key, part):
    return block_elements(jax.random.fold_in(key, 37), NZF // FZ_BLK, FZ_BLK, EZ_BLK)


def block_scale(rng, extent, cuts, least, largest):
    level, own = 1.0, jax.random.fold_in(rng, 6)
    for dim, shards_of in cuts:
        draws = jnp.exp(jax.random.uniform(jax.random.fold_in(own, dim), (shards_of,), jnp.float32, least / len(cuts), largest / len(cuts)))
        level = level * jnp.repeat(draws, extent[dim] // shards_of).reshape([-1 if axis == dim else 1 for axis in range(len(extent))])
    return level


def setup_inputs(seed: int = 0) -> dict:
    streams_of = jax.random.split(jax.random.key(seed), 13)
    return {
        "calcium": jnp.clip(jnp.exp(math.log(3.0) - 3.4011974 * jax.random.uniform(streams_of[0], (SUB, NXF, NZF, NYF), jnp.float32) ** block_scale(streams_of[0], (SUB, NXF, NZF, NYF), ((1, 8), (2, 4), (3, 4)), -0.2, 0.2)), 0.1, 3.0),
        "activation": jnp.clip(1.0 * jax.random.uniform(streams_of[1], (SUB, NXF, NZF, NYF), jnp.float32) ** block_scale(streams_of[1], (SUB, NXF, NZF, NYF), ((1, 8), (2, 4), (3, 4)), -0.2, 0.2), 0.0, 1.0),
        "element_first": draw_element_first(jax.random.fold_in(streams_of[12], 71), 0),
        "offset_first": jnp.clip(jax.random.uniform(streams_of[3], (NXF,), jnp.float32, 0.1, 0.9), 0.1, 0.9),
        "element_second": draw_element_second(jax.random.fold_in(streams_of[12], 71), 0),
        "offset_second": jnp.clip(jax.random.uniform(streams_of[5], (NYF,), jnp.float32, 0.1, 0.9), 0.1, 0.9),
        "element_third": draw_element_third(jax.random.fold_in(streams_of[12], 71), 0),
        "offset_third": jnp.clip(jax.random.uniform(streams_of[7], (NZF,), jnp.float32, 0.1, 0.9), 0.1, 0.9),
        "troponin": jnp.clip(1.0 * jax.random.uniform(streams_of[8], (NXC, NZC, NYC), jnp.float32) ** block_scale(streams_of[8], (NXC, NZC, NYC), ((0, 8), (1, 16)), -0.2, 0.2), 0.0, 1.0),
        "tension": jnp.clip(2.0 * jax.random.uniform(streams_of[9], (NXC, NZC, NYC), jnp.float32) ** block_scale(streams_of[9], (NXC, NZC, NYC), ((0, 8), (1, 16)), -0.2, 0.2), 0.0, 2.0),
        "unbind_rate": jnp.clip(jnp.exp(math.log(2.0) - 2.3025851 * jax.random.uniform(streams_of[10], (NXC, NZC, NYC), jnp.float32) ** block_scale(streams_of[10], (NXC, NZC, NYC), ((0, 8), (1, 16)), -0.2, 0.2)), 0.2, 2.0),
        "relax_rate": jnp.clip(jnp.exp(math.log(4.0) - 2.0794415 * jax.random.uniform(streams_of[11], (NXC, NZC, NYC), jnp.float32) ** block_scale(streams_of[11], (NXC, NZC, NYC), ((0, 8), (1, 16)), -0.2, 0.2)), 0.5, 4.0),
    }


highest = lax.Precision.HIGHEST
step_size = 0.2
bind_rate = 2.0
peak_tension = 2.0
half_square = 0.25


def weights(element, offset, count):
    node_ids = jnp.arange(count, dtype=jnp.int32)
    inside = element[None, :] == node_ids[:, None]
    following = element[None, :] + 1 == node_ids[:, None]
    raw_weights = jnp.where(inside, 1.0 - offset[None, :], 0.0) + jnp.where(following, offset[None, :], 0.0)
    return raw_weights / jnp.sum(raw_weights, axis=1, keepdims=True)


def restrict(field, weight_row, weight_depth, weight_col):
    section = jnp.einsum("ai,izy->azy", weight_row, field, precision=highest)
    section = jnp.einsum("bz,azy->aby", weight_depth, section, precision=highest)
    return jnp.einsum("cy,aby->abc", weight_col, section, precision=highest)


def reference(calcium, activation, element_first, offset_first, element_second, offset_second, element_third, offset_third, troponin, tension, unbind_rate, relax_rate):
    weight_row = weights(element_first, offset_first, NXC)
    weight_col = weights(element_second, offset_second, NYC)
    weight_depth = weights(element_third, offset_third, NZC)

    def single(index):
        return (restrict(calcium[index], weight_row, weight_depth, weight_col),
                restrict(activation[index], weight_row, weight_depth, weight_col))

    drive_calcium, drive_activation = lax.map(single, jnp.arange(SUB, dtype=jnp.int32))
    bound = troponin
    active = tension
    for substep in range(SUB):
        calcium_now = drive_calcium[substep]
        squared = calcium_now * calcium_now
        binding = squared / (squared + half_square)
        bound = bound + step_size * (bind_rate * binding * (1.0 - bound) - unbind_rate * bound)
        active = active + step_size * relax_rate * (peak_tension * drive_activation[substep] * bound - active)
    return bound, active
```

```python
import functools

import jax
import jax.numpy as jnp
from jax import lax
from jax.experimental import pallas as pl
from jax.experimental.pallas import tpu as pltpu
from jax.sharding import PartitionSpec as P

step_size = 0.2
bind_rate = 2.0
peak_tension = 2.0
half_square = 0.25
MESH = pl.DeviceIdType.MESH
f32 = jnp.float32
bf16 = jnp.bfloat16

SLABS = 4
BLOCKS = 4
ROWS = 32
CHUNKS = 4
MAIN = CHUNKS * 16 + 16
EDGE = CHUNKS * 8 + 8


def raw_weights(element, offset, node):
    return jnp.where(element == node, 1.0 - offset, 0.0) + jnp.where(
        element + 1 == node, offset, 0.0
    )


def split(x):
    high = x.astype(bf16)
    low = (x - high.astype(f32)).astype(bf16)
    return high, low


def dot(a, b):
    return jnp.dot(a, b, preferred_element_type=f32)


def iota(shape, dim):
    return lax.broadcasted_iota(jnp.int32, shape, dim)


def spread(element, offset, pick):
    cells = element.shape[1]
    first = offset.astype(bf16).astype(f32)
    second = (offset - first).astype(bf16).astype(f32)
    third = offset - first - second
    row = iota((16, cells), 0)
    stack = jnp.where(
        row == 0,
        element.astype(f32),
        jnp.where(row == 1, first, jnp.where(row == 2, second, jnp.where(row == 3, third, 0.0))),
    )
    out = dot(stack.astype(bf16), pick)
    return out[0:1], out[1:2] + out[2:3] + out[3:4]


def kernel(
    cal, act, ef, of, es, os_, et, ot, trop, tens, unb, rel,
    out_bound, out_active,
    x_buf, ef_v, of_v, es_v, os_v, et_v, ot_v, trop_v, tens_v, unb_v, rel_v,
    w1, w2h, w2l,
    s_main, s_x, s_edge, s_corner,
    r_main, r_x, r_edge, r_corner,
    sem_x, sem_small,
    ss_main, ss_x, ss_edge, ss_corner,
    rs_main, rs_x, rs_edge, rs_corner,
):
    gx, gy, gz = lax.axis_index("gx"), lax.axis_index("gy"), lax.axis_index("gz")
    last_x = lax.axis_size("gx") - 1
    blocks = [lax.rem(gz + 1 + j, BLOCKS) for j in range(BLOCKS)]

    smalls = [
        pltpu.make_async_copy(src, dst, sem_small.at[n])
        for n, (src, dst) in enumerate(
            [(ef, ef_v), (of, of_v), (et, et_v), (ot, ot_v), (es, es_v), (os_, os_v),
             (trop, trop_v), (tens, tens_v), (unb, unb_v), (rel, rel_v)]
        )
    ]
    for copy in smalls:
        copy.start()
    loads = {}
    for j in range(BLOCKS):
        first_cell = pl.multiple_of(blocks[j] * 8, 8)
        for u in range(CHUNKS):
            src = (cal, act)[u // 2].at[pl.ds(4 * (u % 2), 4), :, pl.ds(first_cell, 8), :]
            loads[j, u] = pltpu.make_async_copy(src, x_buf.at[j, u], sem_x.at[j, u])
            loads[j, u].start()

    from_below = jnp.logical_and(gz == 0, gy > 0)
    has_edge = jnp.logical_or(from_below, gz == gy + 1)
    has_x = gx > 0
    sends_x = gx < last_x
    sends_edge = gz < SLABS - 1

    def main_self(c):
        return jnp.logical_and(gy == gz, gy == c)

    def below_self(c):
        return jnp.logical_and(jnp.logical_and(gy == 1, gz == 0), gy == c)

    barrier = pltpu.get_barrier_semaphore()

    def ready(x, y, z):
        pl.semaphore_signal(
            barrier, inc=1, device_id={"gx": x, "gy": y, "gz": z}, device_id_type=MESH
        )

    for c in range(4):
        @pl.when(jnp.logical_not(main_self(c)))
        def _():
            ready(gx, c, gy)

        @pl.when(jnp.logical_and(from_below, jnp.logical_not(below_self(c))))
        def _():
            ready(gx, c, gy - 1)

        @pl.when(has_x)
        def _():
            ready(gx - 1, c, gy)

        @pl.when(jnp.logical_and(has_x, from_below))
        def _():
            ready(gx - 1, c, gy - 1)

    edge_self = jnp.logical_and(gz == 0, gy == 1)
    expected = (
        jnp.where(gy == gz, 3, 4)
        + jnp.where(sends_x, 4, 0)
        + jnp.where(jnp.logical_and(sends_edge, jnp.logical_not(edge_self)), 1, 0)
        + jnp.where(jnp.logical_and(sends_edge, sends_x), 1, 0)
    )

    @pl.when(jnp.logical_not(has_x))
    def _():
        r_x[...] = jnp.zeros_like(r_x)

    @pl.when(jnp.logical_not(has_edge))
    def _():
        r_edge[...] = jnp.zeros_like(r_edge)

    @pl.when(jnp.logical_not(jnp.logical_and(has_x, has_edge)))
    def _():
        r_corner[...] = jnp.zeros_like(r_corner)

    row = iota((ROWS, 1), 0)
    a_of = jnp.where(row < 24, lax.rem(row, 8), 8)
    b_of = jnp.where(row < 24, row // 8, row - 24)
    valid = row < 27
    pick_first = jnp.where(iota((256, 256), 0) == 32 * gx + iota((256, 256), 1) // 8, 1.0, 0.0).astype(bf16)
    pick_cell = iota((128, 256), 0) - lax.rem(iota((128, 256), 1), 8)
    for n in range(4):
        smalls[n].wait()
    e_first = jnp.concatenate([ef_v[0:1, :], ef_v[1:2, :]], axis=1)
    o_first = jnp.concatenate([of_v[0:1, :], of_v[1:2, :]], axis=1)
    node_first = 8 * gx + a_of
    sum_first = jnp.sum(raw_weights(e_first, o_first, node_first), axis=1, keepdims=True)
    ex, ox = spread(e_first, o_first, pick_first)
    wide_first = raw_weights(ex, ox, node_first.astype(f32))
    e_third, o_third = et_v[...], ot_v[...]
    for j in range(BLOCKS):
        node_third = 8 * gz + 2 * blocks[j] + b_of
        sum_third = jnp.sum(raw_weights(e_third, o_third, node_third), axis=1, keepdims=True)
        pick = jnp.where(pick_cell == 32 * gz + 8 * blocks[j], 1.0, 0.0).astype(bf16)
        ex, ox = spread(e_third, o_third, pick)
        scale = jnp.where(valid, 1.0 / jnp.where(valid, sum_first * sum_third, 1.0), 0.0)
        wide = wide_first * raw_weights(ex, ox, node_third.astype(f32)) * scale
        high, low = split(wide)
        w1[j, 0:ROWS] = high
        w1[j, ROWS:] = low

    smalls[4].wait()
    smalls[5].wait()
    node_row = iota((40, 1), 0)
    node_second = 32 * gy + node_row
    inside = jnp.logical_and(node_row < 33, node_second < 128)
    total = jnp.zeros((40, 1), f32)
    for n in range(4):
        total += jnp.sum(
            raw_weights(es_v[n : n + 1, :], os_v[n : n + 1, :], node_second), axis=1, keepdims=True
        )
    own = raw_weights(es_v[pl.ds(gy, 1), :], os_v[pl.ds(gy, 1), :], node_second)
    own = jnp.where(inside, own / jnp.where(inside, total, 1.0), 0.0)
    lane_w = iota((128, 128), 1)
    turned = jnp.transpose(jnp.concatenate([own[0:32]] * 4, axis=0))
    turned_edge = jnp.transpose(jnp.broadcast_to(own[32:33], (128, 128)))
    for k in range(4):
        group = lax.rem(gy + k, 4)
        edge_lane = 32 * lax.rem(gy + 1 + k, 4)
        wide = jnp.concatenate(
            [
                jnp.where(lane_w // 32 == group, turned, 0.0),
                jnp.where(lane_w == edge_lane, turned_edge, 0.0),
            ],
            axis=1,
        )
        high, low = split(wide)
        w2h[128 * k : 128 * (k + 1), :] = high
        w2l[128 * k : 128 * (k + 1), :] = low

    def remote(src, dst, send_sem, recv_sem, x, y, z):
        return pltpu.make_async_remote_copy(
            src_ref=src, dst_ref=dst, send_sem=send_sem, recv_sem=recv_sem,
            device_id={"gx": x, "gy": y, "gz": z}, device_id_type=MESH,
        )

    pending = []

    def send(when, copy):
        @pl.when(when)
        def _():
            copy.start()

        pending.append((when, copy))

    always = gx >= 0
    sub8 = iota((8, 128), 0)
    carry = None
    for j in range(BLOCKS):
        block = blocks[j]
        ys = []
        for u in range(CHUNKS):
            loads[j, u].wait()
            halves = []
            for pair in range(2):
                x = jnp.concatenate(
                    [x_buf[j, u, 2 * pair + n].reshape(256, 128) for n in range(2)], axis=1
                )
                high, low = split(x)
                both = dot(w1[j], high)
                halves.append(both[0:ROWS] + both[ROWS:] + dot(w1[j, 0:ROWS], low))
            ys.append(jnp.concatenate(halves, axis=1))
        y = jnp.concatenate(ys, axis=0)
        high, low = split(y)
        n = CHUNKS * ROWS
        both = dot(jnp.concatenate([high, low], axis=0), w2h[...])
        z = both[0:n] + both[n:] + dot(high, w2l[...])
        parts = [z[ROWS * u : ROWS * (u + 1), 0:128] for u in range(CHUNKS)]
        extra = z[0:ROWS, 128:256]
        for u in range(1, CHUNKS):
            extra += pltpu.roll(z[ROWS * u : ROWS * (u + 1), 128:256], u, axis=1)
        parts.append(extra)
        if carry is not None:
            use = block != 0
            merged = []
            for part, (rows8, corner) in zip(parts, carry):
                merged.append(
                    jnp.concatenate(
                        [
                            part[0:8] + jnp.where(use, rows8, 0.0),
                            part[8:24],
                            part[24:32] + jnp.where(jnp.logical_and(use, sub8 == 0), corner, 0.0),
                        ],
                        axis=0,
                    )
                )
            parts = merged
        carry = [(part[16:24], pltpu.roll(part[24:32], 6, axis=0)) for part in parts]
        for u in range(CHUNKS + 1):
            s_main[j, 16 * u : 16 * (u + 1), :] = parts[u][0:16]
            s_x[j, 2 * u : 2 * (u + 1), :] = parts[u][24:26]

        def store_edge(slot):
            for u in range(CHUNKS + 1):
                s_edge[slot, 8 * u : 8 * (u + 1), :] = parts[u][16:24]
                s_corner[slot, u : u + 1, :] = parts[u][26:27]

        up = jnp.logical_and(block == BLOCKS - 1, sends_edge)

        @pl.when(up)
        def _():
            store_edge(0)

        if j == BLOCKS - 1:
            @pl.when(sends_edge)
            def _():
                store_edge(1)

        if j == 0:
            pl.semaphore_wait(barrier, expected)

        send(
            sends_x,
            remote(s_x.at[j], r_x.at[gy], ss_x.at[j], rs_x.at[gy], gx + 1, gz, block),
        )
        main_copy = remote(
            s_main.at[j], r_main.at[gy], ss_main.at[j], rs_main.at[gy], gx, gz, block
        )
        if j < BLOCKS - 1:
            send(always, main_copy)
        else:
            send(gy != gz, main_copy)

            @pl.when(gy == gz)
            def _():
                r_main[pl.ds(gy, 1)] = s_main[pl.ds(j, 1)]

        @pl.when(jnp.logical_and(up, sends_x))
        def _():
            remote(
                s_corner.at[0], r_corner.at[gy], ss_corner.at[0], rs_corner.at[gy], gx + 1, gz + 1, 0
            ).start()

        @pl.when(jnp.logical_and(up, jnp.logical_not(edge_self)))
        def _():
            remote(
                s_edge.at[0], r_edge.at[gy], ss_edge.at[0], rs_edge.at[gy], gx, gz + 1, 0
            ).start()

        @pl.when(jnp.logical_and(up, edge_self))
        def _():
            r_edge[pl.ds(gy, 1)] = s_edge[0:1]

        if j == BLOCKS - 1:
            send(
                jnp.logical_and(sends_edge, sends_x),
                remote(
                    s_corner.at[1], r_corner.at[gy], ss_corner.at[1], rs_corner.at[gy],
                    gx + 1, gz, gz + 1,
                ),
            )
            send(
                sends_edge,
                remote(
                    s_edge.at[1], r_edge.at[gy], ss_edge.at[1], rs_edge.at[gy], gx, gz, gz + 1
                ),
            )

    pending.append((
        jnp.logical_and(sends_edge, sends_x),
        remote(s_corner.at[0], r_corner.at[gy], ss_corner.at[0], rs_corner.at[gy], gx + 1, gz + 1, 0),
    ))
    pending.append((
        jnp.logical_and(sends_edge, jnp.logical_not(edge_self)),
        remote(s_edge.at[0], r_edge.at[gy], ss_edge.at[0], rs_edge.at[gy], gx, gz + 1, 0),
    ))

    def arrive(when, buf, sems, c, source):
        @pl.when(when)
        def _():
            remote(source, buf.at[c], ss_main.at[0], sems.at[c], gx, gy, gz).wait_recv()

    for c in range(4):
        arrive(jnp.logical_not(main_self(c)), r_main, rs_main, c, s_main.at[0])
        arrive(jnp.logical_and(has_edge, jnp.logical_not(below_self(c))), r_edge, rs_edge, c, s_edge.at[0])
        arrive(has_x, r_x, rs_x, c, s_x.at[0])
        arrive(jnp.logical_and(has_x, has_edge), r_corner, rs_corner, c, s_corner.at[0])
    for n in range(6, 10):
        smalls[n].wait()

    top = sub8 == 0
    lane = iota((8, 128), 1)
    group = lane // 32
    lead = lax.rem(lane, 32) == 0

    def gathered(c, u):
        low_rows = (
            r_main[c, 16 * u : 16 * u + 8, :]
            + r_edge[c, 8 * u : 8 * u + 8, :]
            + jnp.where(top, r_x[c, 2 * u : 2 * u + 1, :] + r_corner[c, u : u + 1, :], 0.0)
        )
        high_rows = r_main[c, 16 * u + 8 : 16 * u + 16, :] + jnp.where(
            top, r_x[c, 2 * u + 1 : 2 * u + 2, :], 0.0
        )
        return low_rows, high_rows

    def by_group(values, shift):
        out = values[(0 - shift) % 4]
        for h in range(1, 4):
            out = jnp.where(group == h, values[(h - shift) % 4], out)
        return out

    extras = [gathered(c, CHUNKS) for c in range(4)]
    drive = {}
    for u in range(CHUNKS):
        mains = [gathered(c, u) for c in range(4)]
        for b in range(2):
            edges = [
                pltpu.roll(extras[c][b], 128 - u, axis=1) if u else extras[c][b] for c in range(4)
            ]
            edges = [jnp.where(lead, value, 0.0) for value in edges]
            for k in range(4):
                value = by_group([mains[c][b] for c in range(4)], k) + by_group(edges, k + 1)
                if k:
                    value = pltpu.roll(value, 128 - 32 * k, axis=1)
                drive[u // 2, 4 * (u % 2) + k, b] = value

    for b in range(2):
        bound, active = trop_v[:, b, :], tens_v[:, b, :]
        unbind, relax = unb_v[:, b, :], rel_v[:, b, :]
        for t in range(8):
            squared = drive[0, t, b] * drive[0, t, b]
            binding = squared / (squared + half_square)
            bound = bound + step_size * (bind_rate * binding * (1.0 - bound) - unbind * bound)
            active = active + step_size * relax * (peak_tension * drive[1, t, b] * bound - active)
        out_bound[:, b, :] = bound
        out_active[:, b, :] = active

    for when, copy in pending:
        @pl.when(when)
        def _():
            copy.wait_send()


def per_device(
    calcium, activation,
    element_first, offset_first, element_second, offset_second, element_third, offset_third,
    troponin, tension, unbind_rate, relax_rate,
):
    anywhere = pl.BlockSpec(memory_space=pl.ANY)
    vmem = pl.BlockSpec(memory_space=pltpu.VMEM)
    dma = pltpu.SemaphoreType.DMA
    small = jax.ShapeDtypeStruct(troponin.shape, f32)
    return pl.pallas_call(
        kernel,
        out_shape=(small, small),
        in_specs=[anywhere] * 12,
        out_specs=(vmem, vmem),
        scratch_shapes=[
            pltpu.VMEM((BLOCKS, CHUNKS, 4, 32, 8, 128), f32),
            pltpu.VMEM((2, 128), jnp.int32),
            pltpu.VMEM((2, 128), f32),
            pltpu.VMEM((4, 128), jnp.int32),
            pltpu.VMEM((4, 128), f32),
            pltpu.VMEM((1, 128), jnp.int32),
            pltpu.VMEM((1, 128), f32),
            *[pltpu.VMEM(troponin.shape, f32) for _ in range(4)],
            pltpu.VMEM((BLOCKS, 2 * ROWS, 256), bf16),
            pltpu.VMEM((512, 256), bf16),
            pltpu.VMEM((512, 256), bf16),
            pltpu.VMEM((BLOCKS, MAIN, 128), f32),
            pltpu.VMEM((BLOCKS, 16, 128), f32),
            pltpu.VMEM((2, EDGE, 128), f32),
            pltpu.VMEM((2, 8, 128), f32),
            pltpu.VMEM((4, MAIN, 128), f32),
            pltpu.VMEM((4, 16, 128), f32),
            pltpu.VMEM((4, EDGE, 128), f32),
            pltpu.VMEM((4, 8, 128), f32),
            dma((BLOCKS, CHUNKS)),
            dma((10,)),
            dma((BLOCKS,)),
            dma((BLOCKS,)),
            dma((2,)),
            dma((2,)),
            dma((4,)),
            dma((4,)),
            dma((4,)),
            dma((4,)),
        ],
        compiler_params=pltpu.CompilerParams(collective_id=0, has_side_effects=True),
        name="restrict_and_step",
    )(
        calcium, activation,
        element_first.reshape(2, 128), offset_first.reshape(2, 128),
        element_second.reshape(4, 128), offset_second.reshape(4, 128),
        element_third.reshape(1, 128), offset_third.reshape(1, 128),
        troponin, tension, unbind_rate, relax_rate,
    )


def solution(mesh):
    nodes = P("gx", ("gy", "gz"), None)
    fine = P(None, "gx", "gz", "gy")
    return jax.shard_map(
        per_device,
        mesh=mesh,
        in_specs=(fine, fine, P(), P(), P(), P(), P(), P(), nodes, nodes, nodes, nodes),
        out_specs=(nodes, nodes),
        check_vma=False,
    )
```

```python
import functools

import jax
import jax.numpy as jnp
from jax import lax
from jax.experimental import pallas as pl
from jax.experimental.pallas import tpu as pltpu
from jax.sharding import PartitionSpec as P

step_size = 0.2
bind_rate = 2.0
peak_tension = 2.0
half_square = 0.25
MESH = pl.DeviceIdType.MESH
f32 = jnp.float32
bf16 = jnp.bfloat16

SLABS = 4
BLOCKS = 4
ROWS = 32
CHUNKS = 4
MAIN = CHUNKS * 16 + 16
EDGE = CHUNKS * 8 + 8


def raw_weights(element, offset, node):
    return jnp.where(element == node, 1.0 - offset, 0.0) + jnp.where(
        element + 1 == node, offset, 0.0
    )


def split(x):
    high = x.astype(bf16)
    low = (x - high.astype(f32)).astype(bf16)
    return high, low


def dot(a, b):
    return jnp.dot(a, b, preferred_element_type=f32)


def iota(shape, dim):
    return lax.broadcasted_iota(jnp.int32, shape, dim)


def spread(element, offset, pick):
    cells = element.shape[1]
    first = offset.astype(bf16).astype(f32)
    second = (offset - first).astype(bf16).astype(f32)
    third = offset - first - second
    row = iota((16, cells), 0)
    stack = jnp.where(
        row == 0,
        element.astype(f32),
        jnp.where(row == 1, first, jnp.where(row == 2, second, jnp.where(row == 3, third, 0.0))),
    )
    out = dot(stack.astype(bf16), pick)
    return out[0:1], out[1:2] + out[2:3] + out[3:4]


def kernel(
    cal, act, ef, of, es, os_, et, ot, trop, tens, unb, rel,
    out_bound, out_active,
    x_buf, ef_v, of_v, es_v, os_v, et_v, ot_v, trop_v, tens_v, unb_v, rel_v,
    w1, w2h, w2l,
    s_main, s_x, s_edge, s_corner,
    r_main, r_x, r_edge, r_corner,
    sem_x, sem_small,
    ss_main, ss_x, ss_edge, ss_corner,
    rs_main, rs_x, rs_edge, rs_corner,
):
    gx, gy, gz = lax.axis_index("gx"), lax.axis_index("gy"), lax.axis_index("gz")
    last_x = lax.axis_size("gx") - 1
    blocks = [lax.rem(gz + 1 + j, BLOCKS) for j in range(BLOCKS)]

    smalls = [
        pltpu.make_async_copy(src, dst, sem_small.at[n])
        for n, (src, dst) in enumerate(
            [(ef, ef_v), (of, of_v), (et, et_v), (ot, ot_v), (es, es_v), (os_, os_v),
             (trop, trop_v), (tens, tens_v), (unb, unb_v), (rel, rel_v)]
        )
    ]
    barrier = pltpu.get_barrier_semaphore()

    def ready(x, y, z):
        pl.semaphore_signal(
            barrier, inc=1, device_id={"gx": x, "gy": y, "gz": z}, device_id_type=MESH
        )

    for copy in smalls[:6]:
        copy.start()

    @pl.when(gx > 0)
    def _():
        ready(gx - 1, 0, gy)

    loads = {}
    for j in range(BLOCKS):
        first_cell = pl.multiple_of(blocks[j] * 8, 8)
        for u in range(CHUNKS):
            src = (cal, act)[u // 2].at[pl.ds(4 * (u % 2), 4), :, pl.ds(first_cell, 8), :]
            loads[j, u] = pltpu.make_async_copy(src, x_buf.at[j, u], sem_x.at[j, u])
            loads[j, u].start()
    for copy in smalls[6:]:
        copy.start()

    from_below = jnp.logical_and(gz == 0, gy > 0)
    has_edge = jnp.logical_or(from_below, gz == gy + 1)
    has_x = gx > 0
    sends_x = gx < last_x
    sends_edge = gz < SLABS - 1

    def main_self(c):
        return jnp.logical_and(gy == gz, gy == c)

    def below_self(c):
        return jnp.logical_and(jnp.logical_and(gy == 1, gz == 0), gy == c)

    for c in range(4):
        @pl.when(jnp.logical_not(main_self(c)))
        def _():
            ready(gx, c, gy)

        @pl.when(jnp.logical_and(from_below, jnp.logical_not(below_self(c))))
        def _():
            ready(gx, c, gy - 1)

        if c > 0:
            @pl.when(has_x)
            def _():
                ready(gx - 1, c, gy)

        @pl.when(jnp.logical_and(has_x, from_below))
        def _():
            ready(gx - 1, c, gy - 1)

    edge_self = jnp.logical_and(gz == 0, gy == 1)
    expected = (
        jnp.where(gy == gz, 3, 4)
        + jnp.where(sends_x, 4, 0)
        + jnp.where(jnp.logical_and(sends_edge, jnp.logical_not(edge_self)), 1, 0)
        + jnp.where(jnp.logical_and(sends_edge, sends_x), 1, 0)
    )

    @pl.when(jnp.logical_not(has_x))
    def _():
        r_x[...] = jnp.zeros_like(r_x)

    @pl.when(jnp.logical_not(has_edge))
    def _():
        r_edge[...] = jnp.zeros_like(r_edge)

    @pl.when(jnp.logical_not(jnp.logical_and(has_x, has_edge)))
    def _():
        r_corner[...] = jnp.zeros_like(r_corner)

    row = iota((ROWS, 1), 0)
    a_of = jnp.where(row < 24, lax.rem(row, 8), 8)
    b_of = jnp.where(row < 24, row // 8, row - 24)
    valid = row < 27
    pick_first = jnp.where(iota((256, 256), 0) == 32 * gx + iota((256, 256), 1) // 8, 1.0, 0.0).astype(bf16)
    pick_cell = iota((128, 256), 0) - lax.rem(iota((128, 256), 1), 8)
    for n in range(4):
        smalls[n].wait()
    e_first = jnp.concatenate([ef_v[0:1, :], ef_v[1:2, :]], axis=1)
    o_first = jnp.concatenate([of_v[0:1, :], of_v[1:2, :]], axis=1)
    node_first = 8 * gx + a_of
    sum_first = jnp.sum(raw_weights(e_first, o_first, node_first), axis=1, keepdims=True)
    ex, ox = spread(e_first, o_first, pick_first)
    wide_first = raw_weights(ex, ox, node_first.astype(f32))
    e_third, o_third = et_v[...], ot_v[...]
    for j in range(BLOCKS):
        node_third = 8 * gz + 2 * blocks[j] + b_of
        sum_third = jnp.sum(raw_weights(e_third, o_third, node_third), axis=1, keepdims=True)
        pick = jnp.where(pick_cell == 32 * gz + 8 * blocks[j], 1.0, 0.0).astype(bf16)
        ex, ox = spread(e_third, o_third, pick)
        scale = jnp.where(valid, 1.0 / jnp.where(valid, sum_first * sum_third, 1.0), 0.0)
        wide = wide_first * raw_weights(ex, ox, node_third.astype(f32)) * scale
        high, low = split(wide)
        w1[j, 0:ROWS] = high
        w1[j, ROWS:] = low

    smalls[4].wait()
    smalls[5].wait()
    node_row = iota((40, 1), 0)
    node_second = 32 * gy + node_row
    inside = jnp.logical_and(node_row < 33, node_second < 128)
    total = jnp.zeros((40, 1), f32)
    for n in range(4):
        total += jnp.sum(
            raw_weights(es_v[n : n + 1, :], os_v[n : n + 1, :], node_second), axis=1, keepdims=True
        )
    own = raw_weights(es_v[pl.ds(gy, 1), :], os_v[pl.ds(gy, 1), :], node_second)
    own = jnp.where(inside, own / jnp.where(inside, total, 1.0), 0.0)
    lane_w = iota((128, 128), 1)
    turned = jnp.transpose(jnp.concatenate([own[0:32]] * 4, axis=0))
    turned_edge = jnp.transpose(jnp.broadcast_to(own[32:33], (128, 128)))
    for k in range(4):
        group = lax.rem(gy + k, 4)
        edge_lane = 32 * lax.rem(gy + 1 + k, 4)
        wide = jnp.concatenate(
            [
                jnp.where(lane_w // 32 == group, turned, 0.0),
                jnp.where(lane_w == edge_lane, turned_edge, 0.0),
            ],
            axis=1,
        )
        high, low = split(wide)
        w2h[128 * k : 128 * (k + 1), :] = high
        w2l[128 * k : 128 * (k + 1), :] = low

    def remote(src, dst, send_sem, recv_sem, x, y, z):
        return pltpu.make_async_remote_copy(
            src_ref=src, dst_ref=dst, send_sem=send_sem, recv_sem=recv_sem,
            device_id={"gx": x, "gy": y, "gz": z}, device_id_type=MESH,
        )

    pending = []

    def send(when, copy):
        @pl.when(when)
        def _():
            copy.start()

        pending.append((when, copy))

    always = gx >= 0
    sub8 = iota((8, 128), 0)
    carry = None
    for j in range(BLOCKS):
        block = blocks[j]
        ys = []
        for u in range(CHUNKS):
            loads[j, u].wait()
        for u in range(CHUNKS):
            halves = []
            for pair in range(2):
                x = jnp.concatenate(
                    [x_buf[j, u, 2 * pair + n].reshape(256, 128) for n in range(2)], axis=1
                )
                high, low = split(x)
                both = dot(w1[j], high)
                halves.append(both[0:ROWS] + both[ROWS:] + dot(w1[j, 0:ROWS], low))
            ys.append(jnp.concatenate(halves, axis=1))
        y = jnp.concatenate(ys, axis=0)
        high, low = split(y)
        n = CHUNKS * ROWS
        both = dot(jnp.concatenate([high, low], axis=0), w2h[...])
        z = both[0:n] + both[n:] + dot(high, w2l[...])
        parts = [z[ROWS * u : ROWS * (u + 1), 0:128] for u in range(CHUNKS)]
        extra = z[0:ROWS, 128:256]
        for u in range(1, CHUNKS):
            extra += pltpu.roll(z[ROWS * u : ROWS * (u + 1), 128:256], u, axis=1)
        parts.append(extra)
        if carry is not None:
            use = block != 0
            merged = []
            for part, (rows8, corner) in zip(parts, carry):
                merged.append(
                    jnp.concatenate(
                        [
                            part[0:8] + jnp.where(use, rows8, 0.0),
                            part[8:24],
                            part[24:32] + jnp.where(jnp.logical_and(use, sub8 == 0), corner, 0.0),
                        ],
                        axis=0,
                    )
                )
            parts = merged
        carry = [(part[16:24], pltpu.roll(part[24:32], 6, axis=0)) for part in parts]
        for u in range(CHUNKS + 1):
            s_main[j, 16 * u : 16 * (u + 1), :] = parts[u][0:16]
            s_x[j, 2 * u : 2 * (u + 1), :] = parts[u][24:26]

        def store_edge(slot):
            for u in range(CHUNKS + 1):
                s_edge[slot, 8 * u : 8 * (u + 1), :] = parts[u][16:24]
                s_corner[slot, u : u + 1, :] = parts[u][26:27]

        up = jnp.logical_and(block == BLOCKS - 1, sends_edge)

        @pl.when(up)
        def _():
            store_edge(0)

        if j == BLOCKS - 1:
            @pl.when(sends_edge)
            def _():
                store_edge(1)

        if j == 0:
            pl.semaphore_wait(barrier, expected)

        send(
            sends_x,
            remote(s_x.at[j], r_x.at[gy], ss_x.at[j], rs_x.at[gy], gx + 1, gz, block),
        )
        main_copy = remote(
            s_main.at[j], r_main.at[gy], ss_main.at[j], rs_main.at[gy], gx, gz, block
        )
        if j < BLOCKS - 1:
            send(always, main_copy)
        else:
            send(gy != gz, main_copy)

            @pl.when(gy == gz)
            def _():
                r_main[pl.ds(gy, 1)] = s_main[pl.ds(j, 1)]

        @pl.when(jnp.logical_and(up, sends_x))
        def _():
            remote(
                s_corner.at[0], r_corner.at[gy], ss_corner.at[0], rs_corner.at[gy], gx + 1, gz + 1, 0
            ).start()

        @pl.when(jnp.logical_and(up, jnp.logical_not(edge_self)))
        def _():
            remote(
                s_edge.at[0], r_edge.at[gy], ss_edge.at[0], rs_edge.at[gy], gx, gz + 1, 0
            ).start()

        @pl.when(jnp.logical_and(up, edge_self))
        def _():
            r_edge[pl.ds(gy, 1)] = s_edge[0:1]

        if j == BLOCKS - 1:
            send(
                jnp.logical_and(sends_edge, sends_x),
                remote(
                    s_corner.at[1], r_corner.at[gy], ss_corner.at[1], rs_corner.at[gy],
                    gx + 1, gz, gz + 1,
                ),
            )
            send(
                sends_edge,
                remote(
                    s_edge.at[1], r_edge.at[gy], ss_edge.at[1], rs_edge.at[gy], gx, gz, gz + 1
                ),
            )

    pending.append((
        jnp.logical_and(sends_edge, sends_x),
        remote(s_corner.at[0], r_corner.at[gy], ss_corner.at[0], rs_corner.at[gy], gx + 1, gz + 1, 0),
    ))
    pending.append((
        jnp.logical_and(sends_edge, jnp.logical_not(edge_self)),
        remote(s_edge.at[0], r_edge.at[gy], ss_edge.at[0], rs_edge.at[gy], gx, gz + 1, 0),
    ))

    def arrive(when, buf, sems, c, source):
        @pl.when(when)
        def _():
            remote(source, buf.at[c], ss_main.at[0], sems.at[c], gx, gy, gz).wait_recv()

    for c in range(4):
        arrive(jnp.logical_not(main_self(c)), r_main, rs_main, c, s_main.at[0])
        arrive(jnp.logical_and(has_edge, jnp.logical_not(below_self(c))), r_edge, rs_edge, c, s_edge.at[0])
        arrive(has_x, r_x, rs_x, c, s_x.at[0])
        arrive(jnp.logical_and(has_x, has_edge), r_corner, rs_corner, c, s_corner.at[0])
    for n in range(6, 10):
        smalls[n].wait()

    top = sub8 == 0
    lane = iota((8, 128), 1)
    group = lane // 32
    lead = lax.rem(lane, 32) == 0

    def gathered(c, u):
        low_rows = (
            r_main[c, 16 * u : 16 * u + 8, :]
            + r_edge[c, 8 * u : 8 * u + 8, :]
            + jnp.where(top, r_x[c, 2 * u : 2 * u + 1, :] + r_corner[c, u : u + 1, :], 0.0)
        )
        high_rows = r_main[c, 16 * u + 8 : 16 * u + 16, :] + jnp.where(
            top, r_x[c, 2 * u + 1 : 2 * u + 2, :], 0.0
        )
        return low_rows, high_rows

    def by_group(values, shift):
        out = values[(0 - shift) % 4]
        for h in range(1, 4):
            out = jnp.where(group == h, values[(h - shift) % 4], out)
        return out

    extras = [gathered(c, CHUNKS) for c in range(4)]
    drive = {}
    for u in range(CHUNKS):
        mains = [gathered(c, u) for c in range(4)]
        for b in range(2):
            edges = [
                pltpu.roll(extras[c][b], 128 - u, axis=1) if u else extras[c][b] for c in range(4)
            ]
            edges = [jnp.where(lead, value, 0.0) for value in edges]
            for k in range(4):
                value = by_group([mains[c][b] for c in range(4)], k) + by_group(edges, k + 1)
                if k:
                    value = pltpu.roll(value, 128 - 32 * k, axis=1)
                drive[u // 2, 4 * (u % 2) + k, b] = value

    for b in range(2):
        bound, active = trop_v[:, b, :], tens_v[:, b, :]
        unbind, relax = unb_v[:, b, :], rel_v[:, b, :]
        for t in range(8):
            squared = drive[0, t, b] * drive[0, t, b]
            binding = squared / (squared + half_square)
            bound = bound + step_size * (bind_rate * binding * (1.0 - bound) - unbind * bound)
            active = active + step_size * relax * (peak_tension * drive[1, t, b] * bound - active)
        out_bound[:, b, :] = bound
        out_active[:, b, :] = active

    for when, copy in pending:
        @pl.when(when)
        def _():
            copy.wait_send()


def write_out(bound, active, out_bound, out_active, sems):
    copies = [
        pltpu.make_async_copy(bound, out_bound, sems.at[0]),
        pltpu.make_async_copy(active, out_active, sems.at[1]),
    ]
    for copy in copies:
        copy.start()
    for copy in copies:
        copy.wait()


def per_device(
    calcium, activation,
    element_first, offset_first, element_second, offset_second, element_third, offset_third,
    troponin, tension, unbind_rate, relax_rate,
):
    anywhere = pl.BlockSpec(memory_space=pltpu.HBM)
    vmem = pl.BlockSpec(memory_space=pltpu.VMEM)
    dma = pltpu.SemaphoreType.DMA
    small = jax.ShapeDtypeStruct(troponin.shape, f32)
    kept = pltpu.VMEM(troponin.shape, f32)
    bound, active = pl.pallas_call(
        kernel,
        out_shape=(kept, kept),
        in_specs=[anywhere] * 12,
        out_specs=(vmem, vmem),
        scratch_shapes=[
            pltpu.VMEM((BLOCKS, CHUNKS, 4, 32, 8, 128), f32),
            pltpu.VMEM((2, 128), jnp.int32),
            pltpu.VMEM((2, 128), f32),
            pltpu.VMEM((4, 128), jnp.int32),
            pltpu.VMEM((4, 128), f32),
            pltpu.VMEM((1, 128), jnp.int32),
            pltpu.VMEM((1, 128), f32),
            *[pltpu.VMEM(troponin.shape, f32) for _ in range(4)],
            pltpu.VMEM((BLOCKS, 2 * ROWS, 256), bf16),
            pltpu.VMEM((512, 256), bf16),
            pltpu.VMEM((512, 256), bf16),
            pltpu.VMEM((BLOCKS, MAIN, 128), f32),
            pltpu.VMEM((BLOCKS, 16, 128), f32),
            pltpu.VMEM((2, EDGE, 128), f32),
            pltpu.VMEM((2, 8, 128), f32),
            pltpu.VMEM((4, MAIN, 128), f32),
            pltpu.VMEM((4, 16, 128), f32),
            pltpu.VMEM((4, EDGE, 128), f32),
            pltpu.VMEM((4, 8, 128), f32),
            dma((BLOCKS, CHUNKS)),
            dma((10,)),
            dma((BLOCKS,)),
            dma((BLOCKS,)),
            dma((2,)),
            dma((2,)),
            dma((4,)),
            dma((4,)),
            dma((4,)),
            dma((4,)),
        ],
        compiler_params=pltpu.CompilerParams(
            collective_id=0, has_side_effects=True, vmem_limit_bytes=60 * 1024 * 1024
        ),
        name="restrict_and_step",
    )(
        calcium, activation,
        element_first.reshape(2, 128), offset_first.reshape(2, 128),
        element_second.reshape(4, 128), offset_second.reshape(4, 128),
        element_third.reshape(1, 128), offset_third.reshape(1, 128),
        troponin, tension, unbind_rate, relax_rate,
    )
    return pl.pallas_call(
        write_out,
        out_shape=(small, small),
        in_specs=[vmem, vmem],
        out_specs=(anywhere, anywhere),
        scratch_shapes=[dma((2,))],
        compiler_params=pltpu.CompilerParams(vmem_limit_bytes=2**20),
        name="write_out",
    )(bound, active)


def solution(mesh):
    nodes = P("gx", ("gy", "gz"), None)
    fine = P(None, "gx", "gz", "gy")
    return jax.shard_map(
        per_device,
        mesh=mesh,
        in_specs=(fine, fine, P(), P(), P(), P(), P(), P(), nodes, nodes, nodes, nodes),
        out_specs=(nodes, nodes),
        check_vma=False,
    )
```

```python
import functools

import jax
import jax.numpy as jnp
from jax import lax
from jax.experimental import pallas as pl
from jax.experimental.pallas import tpu as pltpu
from jax.sharding import PartitionSpec as P

step_size = 0.2
bind_rate = 2.0
peak_tension = 2.0
half_square = 0.25
MESH = pl.DeviceIdType.MESH
f32 = jnp.float32
bf16 = jnp.bfloat16

SLABS = 4
BLOCKS = 4
ROWS = 32
CHUNKS = 4
ORDER = (3, 0, 1, 2)
MAIN = CHUNKS * 16 + 16
EDGE = CHUNKS * 8 + 8


def raw_weights(element, offset, node):
    return jnp.where(element == node, 1.0 - offset, 0.0) + jnp.where(
        element + 1 == node, offset, 0.0
    )


def split(x):
    high = x.astype(bf16)
    low = (x - high.astype(f32)).astype(bf16)
    return high, low


def dot(a, b):
    return jnp.dot(a, b, preferred_element_type=f32)


def iota(shape, dim):
    return lax.broadcasted_iota(jnp.int32, shape, dim)


def spread(element, offset, pick):
    cells = element.shape[1]
    first = offset.astype(bf16).astype(f32)
    second = (offset - first).astype(bf16).astype(f32)
    third = offset - first - second
    row = iota((16, cells), 0)
    stack = jnp.where(
        row == 0,
        element.astype(f32),
        jnp.where(row == 1, first, jnp.where(row == 2, second, jnp.where(row == 3, third, 0.0))),
    )
    out = dot(stack.astype(bf16), pick)
    return out[0:1], out[1:2] + out[2:3] + out[3:4]


def kernel(
    cal, act, ef, of, es, os_, et, ot, trop, tens, unb, rel,
    out_bound, out_active,
    x_buf, ef_v, of_v, es_v, os_v, et_v, ot_v, trop_v, tens_v, unb_v, rel_v,
    w1, w2h, w2l, y_buf, tail, extra_buf,
    s_main, s_x, s_edge, s_corner,
    r_main, r_x, r_edge, r_corner,
    sem_x, sem_small,
    ss_main, ss_x, ss_edge, ss_corner,
    rs_main, rs_x, rs_edge, rs_corner,
):
    gx, gy, gz = lax.axis_index("gx"), lax.axis_index("gy"), lax.axis_index("gz")
    last_x = lax.axis_size("gx") - 1
    blocks = ORDER

    smalls = [
        pltpu.make_async_copy(src, dst, sem_small.at[n])
        for n, (src, dst) in enumerate(
            [(ef, ef_v), (of, of_v), (et, et_v), (ot, ot_v), (es, es_v), (os_, os_v),
             (trop, trop_v), (tens, tens_v), (unb, unb_v), (rel, rel_v)]
        )
    ]
    barrier = pltpu.get_barrier_semaphore()

    def ready(x, y, z):
        pl.semaphore_signal(
            barrier, inc=1, device_id={"gx": x, "gy": y, "gz": z}, device_id_type=MESH
        )

    from_below = jnp.logical_and(gz == 0, gy > 0)
    has_edge = jnp.logical_or(from_below, gz == SLABS - 1)
    has_x = gx > 0
    sends_x = gx < last_x
    sends_edge = gz < SLABS - 1

    for c in range(4):
        @pl.when(has_x)
        def _():
            ready(gx - 1, c, gy)

        @pl.when(jnp.logical_and(has_x, from_below))
        def _():
            ready(gx - 1, c, gy - 1)

    for copy in smalls[:6]:
        copy.start()

    @pl.when(jnp.logical_or(gy != gz, gy != 0))
    def _():
        ready(gx, 0, gy)

    loads = {}
    for j in range(BLOCKS):
        first_cell = blocks[j] * 8
        for u in range(CHUNKS):
            src = (cal, act)[u // 2].at[pl.ds(4 * (u % 2), 4), :, pl.ds(first_cell, 8), :]
            loads[j, u] = pltpu.make_async_copy(src, x_buf.at[j, u], sem_x.at[j, u])

    def issue(j):
        for u in range(CHUNKS):
            loads[j, u].start()

    issue(0)
    for copy in smalls[6:]:
        copy.start()

    def main_self(c):
        return jnp.logical_and(gy == gz, gy == c)

    def below_self(c):
        return jnp.logical_and(jnp.logical_and(gy == 1, gz == 0), gy == c)

    last_self = jnp.logical_and(gy == SLABS - 1, gz == SLABS - 1)

    for c in range(4):
        if c > 0:
            @pl.when(jnp.logical_not(main_self(c)))
            def _():
                ready(gx, c, gy)

        @pl.when(jnp.logical_and(from_below, jnp.logical_not(below_self(c))))
        def _():
            ready(gx, c, gy - 1)

    issue(1)
    edge_self = jnp.logical_and(gz == 0, gy == 1)
    expected = (
        jnp.where(gy == gz, 3, 4)
        + jnp.where(sends_x, 4, 0)
        + jnp.where(jnp.logical_and(sends_edge, jnp.logical_not(edge_self)), 1, 0)
        + jnp.where(jnp.logical_and(sends_edge, sends_x), 1, 0)
    )

    @pl.when(jnp.logical_not(has_x))
    def _():
        r_x[...] = jnp.zeros_like(r_x)

    @pl.when(jnp.logical_not(has_edge))
    def _():
        r_edge[...] = jnp.zeros_like(r_edge)

    @pl.when(jnp.logical_not(jnp.logical_and(has_x, has_edge)))
    def _():
        r_corner[...] = jnp.zeros_like(r_corner)

    row = iota((ROWS, 1), 0)
    a_of = jnp.where(row < 24, lax.rem(row, 8), 8)
    b_of = jnp.where(row < 24, row // 8, row - 24)
    valid = row < 27
    pick_first = jnp.where(iota((256, 256), 0) == 32 * gx + iota((256, 256), 1) // 8, 1.0, 0.0).astype(bf16)
    pick_cell = iota((128, 256), 0) - lax.rem(iota((128, 256), 1), 8)
    for n in range(4):
        smalls[n].wait()
    issue(2)
    e_first = jnp.concatenate([ef_v[0:1, :], ef_v[1:2, :]], axis=1)
    o_first = jnp.concatenate([of_v[0:1, :], of_v[1:2, :]], axis=1)
    node_first = 8 * gx + a_of
    sum_first = jnp.sum(raw_weights(e_first, o_first, node_first), axis=1, keepdims=True)
    ex, ox = spread(e_first, o_first, pick_first)
    wide_first = raw_weights(ex, ox, node_first.astype(f32))
    e_third, o_third = et_v[...], ot_v[...]
    for j in range(BLOCKS):
        node_third = 8 * gz + 2 * blocks[j] + b_of
        sum_third = jnp.sum(raw_weights(e_third, o_third, node_third), axis=1, keepdims=True)
        pick = jnp.where(pick_cell == 32 * gz + 8 * blocks[j], 1.0, 0.0).astype(bf16)
        ex, ox = spread(e_third, o_third, pick)
        scale = jnp.where(valid, 1.0 / jnp.where(valid, sum_first * sum_third, 1.0), 0.0)
        wide = wide_first * raw_weights(ex, ox, node_third.astype(f32)) * scale
        high, low = split(wide)
        w1[j, 0:ROWS] = high
        w1[j, ROWS:] = low

    issue(3)
    smalls[4].wait()
    smalls[5].wait()

    def second_weights():
        node_row = iota((40, 1), 0)
        node_second = 32 * gy + node_row
        inside = jnp.logical_and(node_row < 33, node_second < 128)
        total = jnp.zeros((40, 1), f32)
        for n in range(4):
            total += jnp.sum(
                raw_weights(es_v[n : n + 1, :], os_v[n : n + 1, :], node_second), axis=1, keepdims=True
            )
        own = raw_weights(es_v[pl.ds(gy, 1), :], os_v[pl.ds(gy, 1), :], node_second)
        own = jnp.where(inside, own / jnp.where(inside, total, 1.0), 0.0)
        lane_w = iota((128, 128), 1)
        turned = jnp.transpose(jnp.concatenate([own[0:32]] * 4, axis=0))
        turned_edge = jnp.transpose(jnp.broadcast_to(own[32:33], (128, 128)))
        for k in range(4):
            group = lax.rem(gy + k, 4)
            edge_lane = 32 * lax.rem(gy + 1 + k, 4)
            wide = jnp.concatenate(
                [
                    jnp.where(lane_w // 32 == group, turned, 0.0),
                    jnp.where(lane_w == edge_lane, turned_edge, 0.0),
                ],
                axis=1,
            )
            high, low = split(wide)
            w2h[128 * k : 128 * (k + 1), :] = high
            w2l[128 * k : 128 * (k + 1), :] = low

    def remote(src, dst, send_sem, recv_sem, x, y, z):
        return pltpu.make_async_remote_copy(
            src_ref=src, dst_ref=dst, send_sem=send_sem, recv_sem=recv_sem,
            device_id={"gx": x, "gy": y, "gz": z}, device_id_type=MESH,
        )

    copies = {}

    def put(name, block, when, copy):
        rank = {"x": 1, "corner": 2, "edge": 3, "main": 4}[name]
        copies.setdefault(block, []).append((rank, when, copy))

    sub8 = iota((8, 128), 0)

    def first_stage(j, f):
        slot = (2 * j + f) % 2
        for n in range(2):
            u = 2 * f + n
            for pair in range(2):
                x = jnp.concatenate(
                    [x_buf[j, u, 2 * pair + m].reshape(256, 128) for m in range(2)], axis=1
                )
                high, low = split(x)
                twice = dot(w1[j], high)
                y = twice[0:ROWS] + twice[ROWS:] + dot(w1[j, 0:ROWS], low)
                high, low = split(y)
                columns = slice(256 * pair, 256 * (pair + 1))
                y_buf[slot, ROWS * n : ROWS * (n + 1), columns] = high
                y_buf[slot, ROWS * (2 + n) : ROWS * (3 + n), columns] = low

    def finish(j, u, part):
        if blocks[j] > 0 and j > 0:
            corner = pltpu.roll(tail[u, 8:16, :], 6, axis=0)
            part = [
                part[0:8] + tail[u, 0:8, :],
                part[8:16],
                part[16:24],
                part[24:32] + jnp.where(sub8 == 0, corner, 0.0),
            ]
        else:
            part = [part[8 * n : 8 * (n + 1)] for n in range(4)]
        if j < BLOCKS - 1:
            tail[u, 0:8, :] = part[2]
            tail[u, 8:16, :] = part[3]
        s_main[j, 16 * u : 16 * u + 8, :] = part[0]
        s_main[j, 16 * u + 8 : 16 * u + 16, :] = part[1]
        s_x[j, 2 * u : 2 * (u + 1), :] = part[3][0:2]
        if j in (0, BLOCKS - 1):
            slot = 0 if j == 0 else 1
            s_edge[slot, 8 * u : 8 * (u + 1), :] = part[2]
            s_corner[slot, u : u + 1, :] = part[3][2:3]

    def second_stage(j, f):
        y = y_buf[(2 * j + f) % 2]
        twice = dot(y, w2h[...])
        n = 2 * ROWS
        z = twice[0:n] + twice[n:] + dot(y[0:n], w2l[...])
        extra = 0.0 if f == 0 else extra_buf[...]
        for n in range(2):
            u = 2 * f + n
            rows = z[ROWS * n : ROWS * (n + 1)]
            finish(j, u, rows[:, 0:128])
            extra += pltpu.roll(rows[:, 128:256], u, axis=1) if u else rows[:, 128:256]
        if f == 0:
            extra_buf[...] = extra
        else:
            finish(j, CHUNKS, extra)

    both = jnp.logical_and
    for j, block in enumerate(blocks):
        put("x", j, sends_x, remote(
            s_x.at[j], r_x.at[gy], ss_x.at[j], rs_x.at[gy], gx + 1, gz, block))
        if j == 0:
            put("corner", j, both(sends_edge, sends_x), remote(
                s_corner.at[0], r_corner.at[gy], ss_corner.at[0], rs_corner.at[gy],
                gx + 1, gz + 1, 0))
            put("edge", j, both(sends_edge, jnp.logical_not(edge_self)), remote(
                s_edge.at[0], r_edge.at[gy], ss_edge.at[0], rs_edge.at[gy], gx, gz + 1, 0))
        put("main", j, jnp.logical_not(both(gy == gz, gz == block)), remote(
            s_main.at[j], r_main.at[gy], ss_main.at[j], rs_main.at[gy], gx, gz, block))
        if j == BLOCKS - 1:
            put("corner", j, sends_x, remote(
                s_corner.at[1], r_corner.at[gy], ss_corner.at[1], rs_corner.at[gy],
                gx + 1, gz, BLOCKS - 1))
            put("edge", j, jnp.logical_not(last_self), remote(
                s_edge.at[1], r_edge.at[gy], ss_edge.at[1], rs_edge.at[gy],
                gx, gz, BLOCKS - 1))

    def send_blocks(js, when=None):
        ordered = [pair for j in js for pair in copies[j]]
        for _, condition, copy in sorted(ordered, key=lambda pair: pair[0]):
            condition = condition if when is None else both(condition, when)

            @pl.when(condition)
            def _():
                copy.start()

    late = gz == 0
    early = jnp.logical_not(late)
    EARLY = 4
    for h in range(2 * BLOCKS):
        j, f = h // 2, h % 2
        for u in range(2 * f, 2 * f + 2):
            loads[j, u].wait()
        if h == 0:
            second_weights()
        else:
            second_stage((h - 1) // 2, (h - 1) % 2)
        first_stage(j, f)
        if h == EARLY:
            @pl.when(early)
            def _():
                pl.semaphore_wait(barrier, expected)

            send_blocks(range(j), early)
        elif h > EARLY and f == 0:
            send_blocks([j - 1], early)
    second_stage(BLOCKS - 1, 1)

    @pl.when(late)
    def _():
        pl.semaphore_wait(barrier, expected)

    send_blocks(range(BLOCKS - 1), late)
    send_blocks([BLOCKS - 1])

    for j, block in enumerate(blocks):
        @pl.when(both(gy == gz, gz == block))
        def _():
            r_main[pl.ds(gy, 1)] = s_main[j : j + 1]

    @pl.when(both(sends_edge, edge_self))
    def _():
        r_edge[pl.ds(gy, 1)] = s_edge[0:1]

    @pl.when(last_self)
    def _():
        r_edge[pl.ds(gy, 1)] = s_edge[1:2]

    def arrive(when, buf, sems, c, source):
        @pl.when(when)
        def _():
            remote(source, buf.at[c], ss_main.at[0], sems.at[c], gx, gy, gz).wait_recv()

    for c in range(4):
        arrive(jnp.logical_not(main_self(c)), r_main, rs_main, c, s_main.at[0])
        arrive(jnp.logical_and(has_edge, jnp.logical_not(jnp.logical_or(below_self(c), both(last_self, gy == c)))), r_edge, rs_edge, c, s_edge.at[0])
        arrive(has_x, r_x, rs_x, c, s_x.at[0])
        arrive(jnp.logical_and(has_x, has_edge), r_corner, rs_corner, c, s_corner.at[0])
    for n in range(6, 10):
        smalls[n].wait()

    top = sub8 == 0
    lane = iota((8, 128), 1)
    group = lane // 32
    lead = lax.rem(lane, 32) == 0

    def gathered(c, u):
        low_rows = (
            r_main[c, 16 * u : 16 * u + 8, :]
            + r_edge[c, 8 * u : 8 * u + 8, :]
            + jnp.where(top, r_x[c, 2 * u : 2 * u + 1, :] + r_corner[c, u : u + 1, :], 0.0)
        )
        high_rows = r_main[c, 16 * u + 8 : 16 * u + 16, :] + jnp.where(
            top, r_x[c, 2 * u + 1 : 2 * u + 2, :], 0.0
        )
        return low_rows, high_rows

    def by_group(values, shift):
        out = values[(0 - shift) % 4]
        for h in range(1, 4):
            out = jnp.where(group == h, values[(h - shift) % 4], out)
        return out

    extras = [gathered(c, CHUNKS) for c in range(4)]
    drive = {}
    for u in range(CHUNKS):
        mains = [gathered(c, u) for c in range(4)]
        for b in range(2):
            edges = [
                pltpu.roll(extras[c][b], 128 - u, axis=1) if u else extras[c][b] for c in range(4)
            ]
            edges = [jnp.where(lead, value, 0.0) for value in edges]
            for k in range(4):
                value = by_group([mains[c][b] for c in range(4)], k) + by_group(edges, k + 1)
                if k:
                    value = pltpu.roll(value, 128 - 32 * k, axis=1)
                drive[u // 2, 4 * (u % 2) + k, b] = value

    for b in range(2):
        bound, active = trop_v[:, b, :], tens_v[:, b, :]
        unbind, relax = unb_v[:, b, :], rel_v[:, b, :]
        keep_bound = 1.0 - step_size * unbind
        keep_active = 1.0 - step_size * relax
        for t in range(8):
            squared = drive[0, t, b] * drive[0, t, b]
            gain = (step_size * bind_rate) * (squared / (squared + half_square))
            pull = (step_size * peak_tension) * relax * drive[1, t, b]
            bound = bound * (keep_bound - gain) + gain
            active = active * keep_active + pull * bound
        out_bound[:, b, :] = bound
        out_active[:, b, :] = active

    for j in range(BLOCKS):
        for _, when, copy in copies[j]:
            @pl.when(when)
            def _():
                copy.wait_send()


def write_out(bound, active, out_bound, out_active, sems):
    copies = [
        pltpu.make_async_copy(bound, out_bound, sems.at[0]),
        pltpu.make_async_copy(active, out_active, sems.at[1]),
    ]
    for copy in copies:
        copy.start()
    for copy in copies:
        copy.wait()


def per_device(
    calcium, activation,
    element_first, offset_first, element_second, offset_second, element_third, offset_third,
    troponin, tension, unbind_rate, relax_rate,
):
    anywhere = pl.BlockSpec(memory_space=pltpu.HBM)
    vmem = pl.BlockSpec(memory_space=pltpu.VMEM)
    dma = pltpu.SemaphoreType.DMA
    small = jax.ShapeDtypeStruct(troponin.shape, f32)
    kept = pltpu.VMEM(troponin.shape, f32)
    bound, active = pl.pallas_call(
        kernel,
        out_shape=(kept, kept),
        in_specs=[anywhere] * 12,
        out_specs=(vmem, vmem),
        scratch_shapes=[
            pltpu.VMEM((BLOCKS, CHUNKS, 4, 32, 8, 128), f32),
            pltpu.VMEM((2, 128), jnp.int32),
            pltpu.VMEM((2, 128), f32),
            pltpu.VMEM((4, 128), jnp.int32),
            pltpu.VMEM((4, 128), f32),
            pltpu.VMEM((1, 128), jnp.int32),
            pltpu.VMEM((1, 128), f32),
            *[pltpu.VMEM(troponin.shape, f32) for _ in range(4)],
            pltpu.VMEM((BLOCKS, 2 * ROWS, 256), bf16),
            pltpu.VMEM((512, 256), bf16),
            pltpu.VMEM((512, 256), bf16),
            pltpu.VMEM((2, 4 * ROWS, 512), bf16),
            pltpu.VMEM((CHUNKS + 1, 16, 128), f32),
            pltpu.VMEM((ROWS, 128), f32),
            pltpu.VMEM((BLOCKS, MAIN, 128), f32),
            pltpu.VMEM((BLOCKS, 16, 128), f32),
            pltpu.VMEM((2, EDGE, 128), f32),
            pltpu.VMEM((2, 8, 128), f32),
            pltpu.VMEM((4, MAIN, 128), f32),
            pltpu.VMEM((4, 16, 128), f32),
            pltpu.VMEM((4, EDGE, 128), f32),
            pltpu.VMEM((4, 8, 128), f32),
            dma((BLOCKS, CHUNKS)),
            dma((10,)),
            dma((BLOCKS,)),
            dma((BLOCKS,)),
            dma((2,)),
            dma((2,)),
            dma((4,)),
            dma((4,)),
            dma((4,)),
            dma((4,)),
        ],
        compiler_params=pltpu.CompilerParams(
            collective_id=0, has_side_effects=True, vmem_limit_bytes=60 * 1024 * 1024
        ),
        name="restrict_and_step",
    )(
        calcium, activation,
        element_first.reshape(2, 128), offset_first.reshape(2, 128),
        element_second.reshape(4, 128), offset_second.reshape(4, 128),
        element_third.reshape(1, 128), offset_third.reshape(1, 128),
        troponin, tension, unbind_rate, relax_rate,
    )
    return pl.pallas_call(
        write_out,
        out_shape=(small, small),
        in_specs=[vmem, vmem],
        out_specs=(anywhere, anywhere),
        scratch_shapes=[dma((2,))],
        compiler_params=pltpu.CompilerParams(vmem_limit_bytes=2**20),
        name="write_out",
    )(bound, active)


def solution(mesh):
    nodes = P("gx", ("gy", "gz"), None)
    fine = P(None, "gx", "gz", "gy")
    return jax.shard_map(
        per_device,
        mesh=mesh,
        in_specs=(fine, fine, P(), P(), P(), P(), P(), P(), nodes, nodes, nodes, nodes),
        out_specs=(nodes, nodes),
        check_vma=False,
    )
```

```python
import functools

import jax
import jax.numpy as jnp
from jax import lax
from jax.experimental import pallas as pl
from jax.experimental.pallas import tpu as pltpu
from jax.sharding import PartitionSpec as P

step_size = 0.2
bind_rate = 2.0
peak_tension = 2.0
half_square = 0.25
MESH = pl.DeviceIdType.MESH
f32 = jnp.float32
bf16 = jnp.bfloat16

SLABS = 4
BLOCKS = 4
ROWS = 32
CHUNKS = 4
ORDER = (3, 0, 1, 2)
PLACE = (4, 4, 4, 4, 4, 4)
MAIN = CHUNKS * 16 + 16
EDGE = CHUNKS * 8 + 8


def raw_weights(element, offset, node):
    return jnp.where(element == node, 1.0 - offset, 0.0) + jnp.where(
        element + 1 == node, offset, 0.0
    )


def split(x):
    high = x.astype(bf16)
    low = (x - high.astype(f32)).astype(bf16)
    return high, low


def dot(a, b):
    return jnp.dot(a, b, preferred_element_type=f32)


def iota(shape, dim):
    return lax.broadcasted_iota(jnp.int32, shape, dim)


def spread(element, offset, pick):
    cells = element.shape[1]
    first = offset.astype(bf16).astype(f32)
    second = (offset - first).astype(bf16).astype(f32)
    third = offset - first - second
    row = iota((16, cells), 0)
    stack = jnp.where(
        row == 0,
        element.astype(f32),
        jnp.where(row == 1, first, jnp.where(row == 2, second, jnp.where(row == 3, third, 0.0))),
    )
    out = dot(stack.astype(bf16), pick)
    return out[0:1], out[1:2] + out[2:3] + out[3:4]


def kernel(
    cal, act, ef, of, es, os_, et, ot, trop, tens, unb, rel,
    out_bound, out_active,
    x_buf, ef_v, of_v, es_v, os_v, et_v, ot_v, trop_v, tens_v, unb_v, rel_v,
    w1, w2h, w2l, y_buf, tail, extra_buf,
    s_main, s_x, s_edge, s_corner,
    r_main, r_x, r_edge, r_corner,
    sem_x, sem_small,
    ss_main, ss_x, ss_edge, ss_corner,
    rs_main, rs_x, rs_edge, rs_corner, x_ready,
):
    gx, gy, gz = lax.axis_index("gx"), lax.axis_index("gy"), lax.axis_index("gz")
    last_x = lax.axis_size("gx") - 1
    blocks = ORDER

    smalls = [
        pltpu.make_async_copy(src, dst, sem_small.at[n])
        for n, (src, dst) in enumerate(
            [(ef, ef_v), (of, of_v), (et, et_v), (ot, ot_v), (es, es_v), (os_, os_v),
             (trop, trop_v), (tens, tens_v), (unb, unb_v), (rel, rel_v)]
        )
    ]
    barrier = pltpu.get_barrier_semaphore()

    def ready(x, y, z):
        pl.semaphore_signal(
            barrier, inc=1, device_id={"gx": x, "gy": y, "gz": z}, device_id_type=MESH
        )

    from_below = jnp.logical_and(gz == 0, gy > 0)
    has_edge = jnp.logical_or(from_below, gz == SLABS - 1)
    has_x = gx > 0
    sends_x = gx < last_x
    sends_edge = gz < SLABS - 1

    near = gz < 2
    relays = jnp.logical_and(gz >= 2, sends_x)

    for c in range(4):
        @pl.when(jnp.logical_and(has_x, near))
        def _():
            ready(gx - 1, c, gy)

        @pl.when(jnp.logical_and(has_x, from_below))
        def _():
            ready(gx - 1, c, gy - 1)

    @pl.when(jnp.logical_and(has_x, gz >= 2))
    def _():
        ready(gx - 1, gy, gz)

    for q in (2, 3):
        @pl.when(jnp.logical_and(sends_x, jnp.logical_not(jnp.logical_and(gy == gz, gz == q))))
        def _():
            ready(gx, gz, q)

    for copy in smalls[:6]:
        copy.start()

    @pl.when(jnp.logical_or(gy != gz, gy != 0))
    def _():
        ready(gx, 0, gy)

    loads = {}
    for j in range(BLOCKS):
        first_cell = blocks[j] * 8
        for u in range(CHUNKS):
            src = (cal, act)[u // 2].at[pl.ds(4 * (u % 2), 4), :, pl.ds(first_cell, 8), :]
            loads[j, u] = pltpu.make_async_copy(src, x_buf.at[j, u], sem_x.at[j, u])

    def issue(j):
        for u in range(CHUNKS):
            loads[j, u].start()

    issue(0)
    for copy in smalls[6:]:
        copy.start()

    def main_self(c):
        return jnp.logical_and(gy == gz, gy == c)

    def below_self(c):
        return jnp.logical_and(jnp.logical_and(gy == 1, gz == 0), gy == c)

    last_self = jnp.logical_and(gy == SLABS - 1, gz == SLABS - 1)

    for c in range(4):
        if c > 0:
            @pl.when(jnp.logical_not(main_self(c)))
            def _():
                ready(gx, c, gy)

        @pl.when(jnp.logical_and(from_below, jnp.logical_not(below_self(c))))
        def _():
            ready(gx, c, gy - 1)

    issue(1)
    edge_self = jnp.logical_and(gz == 0, gy == 1)
    expected = (
        jnp.where(gy == gz, 3, 4)
        + jnp.where(sends_x, 2, 0)
        + jnp.where(relays, jnp.where(gy == gz, 4, 5), 0)
        + jnp.where(jnp.logical_and(sends_edge, jnp.logical_not(edge_self)), 1, 0)
        + jnp.where(jnp.logical_and(sends_edge, sends_x), 1, 0)
    )

    @pl.when(jnp.logical_not(has_x))
    def _():
        r_x[...] = jnp.zeros_like(r_x)

    @pl.when(jnp.logical_not(has_edge))
    def _():
        r_edge[...] = jnp.zeros_like(r_edge)

    @pl.when(jnp.logical_not(jnp.logical_and(has_x, has_edge)))
    def _():
        r_corner[...] = jnp.zeros_like(r_corner)

    row = iota((ROWS, 1), 0)
    a_of = jnp.where(row < 24, lax.rem(row, 8), 8)
    b_of = jnp.where(row < 24, row // 8, row - 24)
    valid = row < 27
    pick_first = jnp.where(iota((256, 256), 0) == 32 * gx + iota((256, 256), 1) // 8, 1.0, 0.0).astype(bf16)
    pick_cell = iota((128, 256), 0) - lax.rem(iota((128, 256), 1), 8)
    for n in range(4):
        smalls[n].wait()
    issue(2)
    e_first = jnp.concatenate([ef_v[0:1, :], ef_v[1:2, :]], axis=1)
    o_first = jnp.concatenate([of_v[0:1, :], of_v[1:2, :]], axis=1)
    node_first = 8 * gx + a_of
    sum_first = jnp.sum(raw_weights(e_first, o_first, node_first), axis=1, keepdims=True)
    ex, ox = spread(e_first, o_first, pick_first)
    wide_first = raw_weights(ex, ox, node_first.astype(f32))
    e_third, o_third = et_v[...], ot_v[...]
    for j in range(BLOCKS):
        node_third = 8 * gz + 2 * blocks[j] + b_of
        sum_third = jnp.sum(raw_weights(e_third, o_third, node_third), axis=1, keepdims=True)
        pick = jnp.where(pick_cell == 32 * gz + 8 * blocks[j], 1.0, 0.0).astype(bf16)
        ex, ox = spread(e_third, o_third, pick)
        scale = jnp.where(valid, 1.0 / jnp.where(valid, sum_first * sum_third, 1.0), 0.0)
        wide = wide_first * raw_weights(ex, ox, node_third.astype(f32)) * scale
        high, low = split(wide)
        w1[j, 0:ROWS] = high
        w1[j, ROWS:] = low

    issue(3)
    smalls[4].wait()
    smalls[5].wait()

    def second_weights():
        node_row = iota((40, 1), 0)
        node_second = 32 * gy + node_row
        inside = jnp.logical_and(node_row < 33, node_second < 128)
        total = jnp.zeros((40, 1), f32)
        for n in range(4):
            total += jnp.sum(
                raw_weights(es_v[n : n + 1, :], os_v[n : n + 1, :], node_second), axis=1, keepdims=True
            )
        own = raw_weights(es_v[pl.ds(gy, 1), :], os_v[pl.ds(gy, 1), :], node_second)
        own = jnp.where(inside, own / jnp.where(inside, total, 1.0), 0.0)
        lane_w = iota((128, 128), 1)
        turned = jnp.transpose(jnp.concatenate([own[0:32]] * 4, axis=0))
        turned_edge = jnp.transpose(jnp.broadcast_to(own[32:33], (128, 128)))
        for k in range(4):
            group = lax.rem(gy + k, 4)
            edge_lane = 32 * lax.rem(gy + 1 + k, 4)
            wide = jnp.concatenate(
                [
                    jnp.where(lane_w // 32 == group, turned, 0.0),
                    jnp.where(lane_w == edge_lane, turned_edge, 0.0),
                ],
                axis=1,
            )
            high, low = split(wide)
            w2h[128 * k : 128 * (k + 1), :] = high
            w2l[128 * k : 128 * (k + 1), :] = low

    def remote(src, dst, send_sem, recv_sem, x, y, z):
        return pltpu.make_async_remote_copy(
            src_ref=src, dst_ref=dst, send_sem=send_sem, recv_sem=recv_sem,
            device_id={"gx": x, "gy": y, "gz": z}, device_id_type=MESH,
        )

    sub8 = iota((8, 128), 0)

    def first_stage(j, f):
        slot = (2 * j + f) % 2
        for n in range(2):
            u = 2 * f + n
            for pair in range(2):
                x = jnp.concatenate(
                    [x_buf[j, u, 2 * pair + m].reshape(256, 128) for m in range(2)], axis=1
                )
                high, low = split(x)
                twice = dot(w1[j], high)
                y = twice[0:ROWS] + twice[ROWS:] + dot(w1[j, 0:ROWS], low)
                high, low = split(y)
                columns = slice(256 * pair, 256 * (pair + 1))
                y_buf[slot, ROWS * n : ROWS * (n + 1), columns] = high
                y_buf[slot, ROWS * (2 + n) : ROWS * (3 + n), columns] = low

    def finish(j, u, part):
        if blocks[j] > 0 and j > 0:
            corner = pltpu.roll(tail[u, 8:16, :], 6, axis=0)
            part = [
                part[0:8] + tail[u, 0:8, :],
                part[8:16],
                part[16:24],
                part[24:32] + jnp.where(sub8 == 0, corner, 0.0),
            ]
        else:
            part = [part[8 * n : 8 * (n + 1)] for n in range(4)]
        if j < BLOCKS - 1:
            tail[u, 0:8, :] = part[2]
            tail[u, 8:16, :] = part[3]
        s_main[j, 16 * u : 16 * u + 8, :] = part[0]
        s_main[j, 16 * u + 8 : 16 * u + 16, :] = part[1]
        s_x[j, 2 * u : 2 * (u + 1), :] = part[3][0:2]
        if j in (0, BLOCKS - 1):
            slot = 0 if j == 0 else 1
            s_edge[slot, 8 * u : 8 * (u + 1), :] = part[2]
            s_corner[slot, u : u + 1, :] = part[3][2:3]

    def second_stage(j, f):
        y = y_buf[(2 * j + f) % 2]
        twice = dot(y, w2h[...])
        n = 2 * ROWS
        z = twice[0:n] + twice[n:] + dot(y[0:n], w2l[...])
        extra = 0.0 if f == 0 else extra_buf[...]
        for n in range(2):
            u = 2 * f + n
            rows = z[ROWS * n : ROWS * (n + 1)]
            finish(j, u, rows[:, 0:128])
            extra += pltpu.roll(rows[:, 128:256], u, axis=1) if u else rows[:, 128:256]
        if f == 0:
            extra_buf[...] = extra
        else:
            finish(j, CHUNKS, extra)

    both = jnp.logical_and
    copies = {}
    for j, block in enumerate(blocks):
        copies["x", j] = (sends_x, remote(
            s_x.at[j], r_x.at[gy], ss_x.at[j], rs_x.at[gy], gx + 1, gz, block))
        if j == 0:
            copies["corner", 0] = (both(sends_edge, sends_x), remote(
                s_corner.at[0], r_corner.at[gy], ss_corner.at[0], rs_corner.at[gy],
                gx + 1, gz + 1, 0))
            copies["edge", 0] = (both(sends_edge, jnp.logical_not(edge_self)), remote(
                s_edge.at[0], r_edge.at[gy], ss_edge.at[0], rs_edge.at[gy], gx, gz + 1, 0))
        copies["main", j] = (jnp.logical_not(both(gy == gz, gz == block)), remote(
            s_main.at[j], r_main.at[gy], ss_main.at[j], rs_main.at[gy], gx, gz, block))
        if j == BLOCKS - 1:
            copies["corner", 1] = (sends_x, remote(
                s_corner.at[1], r_corner.at[gy], ss_corner.at[1], rs_corner.at[gy],
                gx + 1, gz, BLOCKS - 1))
            copies["edge", 1] = (jnp.logical_not(last_self), remote(
                s_edge.at[1], r_edge.at[gy], ss_edge.at[1], rs_edge.at[gy],
                gx, gz, BLOCKS - 1))

    READY = [
        [("corner", 0), ("edge", 0), ("main", 0)],
        [("x", 1), ("main", 1)],
        [("x", 2), ("main", 2)],
        [("main", 3), ("edge", 1)],
    ]
    RANK = {"x": 0, "corner": 1, "edge": 2, "main": 3}

    def send(names, when=None):
        for name in names:
            condition, copy = copies[name]
            condition = condition if when is None else both(condition, when)

            @pl.when(condition)
            def _():
                copy.start()

    def enter(when):
        @pl.when(when)
        def _():
            pl.semaphore_wait(barrier, expected)

        for c in range(4):
            @pl.when(both(both(when, relays), jnp.logical_not(main_self(c))))
            def _():
                pl.semaphore_signal(
                    x_ready.at[lax.max(gz - 2, 0)], inc=1,
                    device_id={"gx": gx, "gy": c, "gz": gy}, device_id_type=MESH,
                )

        @pl.when(both(both(when, relays), gy == gz))
        def _():
            pl.semaphore_signal(x_ready.at[lax.max(gz - 2, 0)], inc=1)

    place = jnp.where(gx == 3, jnp.where(gz == 2, PLACE[5], PLACE[4]), jnp.where(
        gz == 0, PLACE[0], jnp.where(gz == 1, PLACE[1], jnp.where(gz == 2, PLACE[2], PLACE[3]))))
    for h in range(2 * BLOCKS + 1):
        j, f = h // 2, h % 2
        if h < 2 * BLOCKS:
            for u in range(2 * f, 2 * f + 2):
                loads[j, u].wait()
        if h == 0:
            second_weights()
        else:
            second_stage((h - 1) // 2, (h - 1) % 2)
        if h < 2 * BLOCKS:
            first_stage(j, f)
        if h in PLACE:
            here = place == h
            enter(here)
            names = [name for i in range(j - 1) for name in READY[i]]
            send(sorted(names, key=lambda name: RANK[name[0]]), here)
        if h >= min(PLACE) and f == 0:
            send(READY[j - 1], place <= h if h < max(PLACE) else None)

    for n, names in ((1, [("x", 0), ("corner", 1)]), (0, [("x", 3)])):
        @pl.when(sends_x)
        def _():
            pl.semaphore_wait(x_ready.at[n], 1)

        send(names)

    for j, block in enumerate(blocks):
        @pl.when(both(gy == gz, gz == block))
        def _():
            r_main[pl.ds(gy, 1)] = s_main[j : j + 1]

    @pl.when(both(sends_edge, edge_self))
    def _():
        r_edge[pl.ds(gy, 1)] = s_edge[0:1]

    @pl.when(last_self)
    def _():
        r_edge[pl.ds(gy, 1)] = s_edge[1:2]

    def arrive(when, buf, sems, c, source):
        @pl.when(when)
        def _():
            remote(source, buf.at[c], ss_main.at[0], sems.at[c], gx, gy, gz).wait_recv()

    for c in range(4):
        arrive(jnp.logical_not(main_self(c)), r_main, rs_main, c, s_main.at[0])
        arrive(jnp.logical_and(has_edge, jnp.logical_not(jnp.logical_or(below_self(c), both(last_self, gy == c)))), r_edge, rs_edge, c, s_edge.at[0])
        arrive(has_x, r_x, rs_x, c, s_x.at[0])
        arrive(jnp.logical_and(has_x, has_edge), r_corner, rs_corner, c, s_corner.at[0])
    for n in range(6, 10):
        smalls[n].wait()

    top = sub8 == 0
    lane = iota((8, 128), 1)
    group = lane // 32
    lead = lax.rem(lane, 32) == 0

    def gathered(c, u):
        low_rows = (
            r_main[c, 16 * u : 16 * u + 8, :]
            + r_edge[c, 8 * u : 8 * u + 8, :]
            + jnp.where(top, r_x[c, 2 * u : 2 * u + 1, :] + r_corner[c, u : u + 1, :], 0.0)
        )
        high_rows = r_main[c, 16 * u + 8 : 16 * u + 16, :] + jnp.where(
            top, r_x[c, 2 * u + 1 : 2 * u + 2, :], 0.0
        )
        return low_rows, high_rows

    def by_group(values, shift):
        out = values[(0 - shift) % 4]
        for h in range(1, 4):
            out = jnp.where(group == h, values[(h - shift) % 4], out)
        return out

    extras = [gathered(c, CHUNKS) for c in range(4)]
    drive = {}
    for u in range(CHUNKS):
        mains = [gathered(c, u) for c in range(4)]
        for b in range(2):
            edges = [
                pltpu.roll(extras[c][b], 128 - u, axis=1) if u else extras[c][b] for c in range(4)
            ]
            edges = [jnp.where(lead, value, 0.0) for value in edges]
            for k in range(4):
                value = by_group([mains[c][b] for c in range(4)], k) + by_group(edges, k + 1)
                if k:
                    value = pltpu.roll(value, 128 - 32 * k, axis=1)
                drive[u // 2, 4 * (u % 2) + k, b] = value

    for b in range(2):
        bound, active = trop_v[:, b, :], tens_v[:, b, :]
        unbind, relax = unb_v[:, b, :], rel_v[:, b, :]
        keep_bound = 1.0 - step_size * unbind
        keep_active = 1.0 - step_size * relax
        for t in range(8):
            squared = drive[0, t, b] * drive[0, t, b]
            gain = (step_size * bind_rate) * (squared / (squared + half_square))
            pull = (step_size * peak_tension) * relax * drive[1, t, b]
            bound = bound * (keep_bound - gain) + gain
            active = active * keep_active + pull * bound
        out_bound[:, b, :] = bound
        out_active[:, b, :] = active

    for when, copy in copies.values():
        @pl.when(when)
        def _():
            copy.wait_send()


def write_out(bound, active, out_bound, out_active, sems):
    copies = [
        pltpu.make_async_copy(bound, out_bound, sems.at[0]),
        pltpu.make_async_copy(active, out_active, sems.at[1]),
    ]
    for copy in copies:
        copy.start()
    for copy in copies:
        copy.wait()


def per_device(
    calcium, activation,
    element_first, offset_first, element_second, offset_second, element_third, offset_third,
    troponin, tension, unbind_rate, relax_rate,
):
    anywhere = pl.BlockSpec(memory_space=pltpu.HBM)
    vmem = pl.BlockSpec(memory_space=pltpu.VMEM)
    dma = pltpu.SemaphoreType.DMA
    small = jax.ShapeDtypeStruct(troponin.shape, f32)
    kept = pltpu.VMEM(troponin.shape, f32)
    bound, active = pl.pallas_call(
        kernel,
        out_shape=(kept, kept),
        in_specs=[anywhere] * 12,
        out_specs=(vmem, vmem),
        scratch_shapes=[
            pltpu.VMEM((BLOCKS, CHUNKS, 4, 32, 8, 128), f32),
            pltpu.VMEM((2, 128), jnp.int32),
            pltpu.VMEM((2, 128), f32),
            pltpu.VMEM((4, 128), jnp.int32),
            pltpu.VMEM((4, 128), f32),
            pltpu.VMEM((1, 128), jnp.int32),
            pltpu.VMEM((1, 128), f32),
            *[pltpu.VMEM(troponin.shape, f32) for _ in range(4)],
            pltpu.VMEM((BLOCKS, 2 * ROWS, 256), bf16),
            pltpu.VMEM((512, 256), bf16),
            pltpu.VMEM((512, 256), bf16),
            pltpu.VMEM((2, 4 * ROWS, 512), bf16),
            pltpu.VMEM((CHUNKS + 1, 16, 128), f32),
            pltpu.VMEM((ROWS, 128), f32),
            pltpu.VMEM((BLOCKS, MAIN, 128), f32),
            pltpu.VMEM((BLOCKS, 16, 128), f32),
            pltpu.VMEM((2, EDGE, 128), f32),
            pltpu.VMEM((2, 8, 128), f32),
            pltpu.VMEM((4, MAIN, 128), f32),
            pltpu.VMEM((4, 16, 128), f32),
            pltpu.VMEM((4, EDGE, 128), f32),
            pltpu.VMEM((4, 8, 128), f32),
            dma((BLOCKS, CHUNKS)),
            dma((10,)),
            dma((BLOCKS,)),
            dma((BLOCKS,)),
            dma((2,)),
            dma((2,)),
            dma((4,)),
            dma((4,)),
            dma((4,)),
            dma((4,)),
            pltpu.SemaphoreType.REGULAR((2,)),
        ],
        compiler_params=pltpu.CompilerParams(
            collective_id=0, has_side_effects=True, vmem_limit_bytes=60 * 1024 * 1024
        ),
        name="restrict_and_step",
    )(
        calcium, activation,
        element_first.reshape(2, 128), offset_first.reshape(2, 128),
        element_second.reshape(4, 128), offset_second.reshape(4, 128),
        element_third.reshape(1, 128), offset_third.reshape(1, 128),
        troponin, tension, unbind_rate, relax_rate,
    )
    return pl.pallas_call(
        write_out,
        out_shape=(small, small),
        in_specs=[vmem, vmem],
        out_specs=(anywhere, anywhere),
        scratch_shapes=[dma((2,))],
        compiler_params=pltpu.CompilerParams(vmem_limit_bytes=2**20),
        name="write_out",
    )(bound, active)


def solution(mesh):
    nodes = P("gx", ("gy", "gz"), None)
    fine = P(None, "gx", "gz", "gy")
    return jax.shard_map(
        per_device,
        mesh=mesh,
        in_specs=(fine, fine, P(), P(), P(), P(), P(), P(), nodes, nodes, nodes, nodes),
        out_specs=(nodes, nodes),
        check_vma=False,
    )
```

```python
import functools

import jax
import jax.numpy as jnp
from jax import lax
from jax.experimental import pallas as pl
from jax.experimental.pallas import tpu as pltpu
from jax.sharding import PartitionSpec as P

step_size = 0.2
bind_rate = 2.0
peak_tension = 2.0
half_square = 0.25
MESH = pl.DeviceIdType.MESH
f32 = jnp.float32
bf16 = jnp.bfloat16

SLABS = 4
BLOCKS = 4
ROWS = 32
CHUNKS = 4
ORDER = (3, 0, 1, 2)
PLACE = (4, 4, 2, 2, 4, 4)
MAIN = CHUNKS * 16 + 2
EDGE = CHUNKS * 8 + 1
CROSS = CHUNKS * 2 + 1
CORNER = CHUNKS + 1


def raw_weights(element, offset, node):
    return jnp.where(element == node, 1.0 - offset, 0.0) + jnp.where(
        element + 1 == node, offset, 0.0
    )


def split(x):
    high = x.astype(bf16)
    low = (x - high.astype(f32)).astype(bf16)
    return high, low


def dot(a, b):
    return jnp.dot(a, b, preferred_element_type=f32)


def iota(shape, dim):
    return lax.broadcasted_iota(jnp.int32, shape, dim)


def spread(element, offset, pick):
    cells = element.shape[1]
    first = offset.astype(bf16).astype(f32)
    second = (offset - first).astype(bf16).astype(f32)
    third = offset - first - second
    row = iota((16, cells), 0)
    stack = jnp.where(
        row == 0,
        element.astype(f32),
        jnp.where(row == 1, first, jnp.where(row == 2, second, jnp.where(row == 3, third, 0.0))),
    )
    out = dot(stack.astype(bf16), pick)
    return out[0:1], out[1:2] + out[2:3] + out[3:4]


def kernel(
    cal, act, ef, of, es, os_, et, ot, trop, tens, unb, rel,
    out_bound, out_active,
    x_buf, ef_v, of_v, es_v, os_v, et_v, ot_v, trop_v, tens_v, unb_v, rel_v,
    w1, w2h, w2l, y_buf, tail, extra_buf,
    s_main, s_x, s_edge, s_corner,
    r_main, r_x, r_edge, r_corner,
    sem_x, sem_small,
    ss_main, ss_x, ss_edge, ss_corner,
    rs_main, rs_x, rs_edge, rs_corner, x_ready,
):
    gx, gy, gz = lax.axis_index("gx"), lax.axis_index("gy"), lax.axis_index("gz")
    last_x = lax.axis_size("gx") - 1
    blocks = ORDER

    smalls = [
        pltpu.make_async_copy(src, dst, sem_small.at[n])
        for n, (src, dst) in enumerate(
            [(ef, ef_v), (of, of_v), (et, et_v), (ot, ot_v), (es, es_v), (os_, os_v),
             (trop, trop_v), (tens, tens_v), (unb, unb_v), (rel, rel_v)]
        )
    ]
    barrier = pltpu.get_barrier_semaphore()

    def ready(x, y, z):
        pl.semaphore_signal(
            barrier, inc=1, device_id={"gx": x, "gy": y, "gz": z}, device_id_type=MESH
        )

    from_below = jnp.logical_and(gz == 0, gy > 0)
    has_edge = jnp.logical_or(from_below, gz == SLABS - 1)
    has_x = gx > 0
    sends_x = gx < last_x
    sends_edge = gz < SLABS - 1

    near = gz < 2
    relays = jnp.logical_and(gz >= 2, sends_x)

    for c in range(4):
        @pl.when(jnp.logical_and(has_x, near))
        def _():
            ready(gx - 1, c, gy)

        @pl.when(jnp.logical_and(has_x, from_below))
        def _():
            ready(gx - 1, c, gy - 1)

    @pl.when(jnp.logical_and(has_x, gz >= 2))
    def _():
        ready(gx - 1, gy, gz)

    for q in (2, 3):
        @pl.when(jnp.logical_and(sends_x, jnp.logical_not(jnp.logical_and(gy == gz, gz == q))))
        def _():
            ready(gx, gz, q)

    for copy in smalls[:6]:
        copy.start()

    @pl.when(jnp.logical_or(gy != gz, gy != 0))
    def _():
        ready(gx, 0, gy)

    loads = {}
    for j in range(BLOCKS):
        first_cell = blocks[j] * 8
        for u in range(CHUNKS):
            src = (cal, act)[u // 2].at[pl.ds(4 * (u % 2), 4), :, pl.ds(first_cell, 8), :]
            loads[j, u] = pltpu.make_async_copy(src, x_buf.at[j, u], sem_x.at[j, u])

    def issue(j):
        for u in range(CHUNKS):
            loads[j, u].start()

    issue(0)
    for copy in smalls[6:]:
        copy.start()

    def main_self(c):
        return jnp.logical_and(gy == gz, gy == c)

    def below_self(c):
        return jnp.logical_and(jnp.logical_and(gy == 1, gz == 0), gy == c)

    last_self = jnp.logical_and(gy == SLABS - 1, gz == SLABS - 1)

    for c in range(4):
        if c > 0:
            @pl.when(jnp.logical_not(main_self(c)))
            def _():
                ready(gx, c, gy)

        @pl.when(jnp.logical_and(from_below, jnp.logical_not(below_self(c))))
        def _():
            ready(gx, c, gy - 1)

    issue(1)
    edge_self = jnp.logical_and(gz == 0, gy == 1)
    expected = (
        jnp.where(gy == gz, 3, 4)
        + jnp.where(sends_x, 2, 0)
        + jnp.where(relays, jnp.where(gy == gz, 4, 5), 0)
        + jnp.where(jnp.logical_and(sends_edge, jnp.logical_not(edge_self)), 1, 0)
        + jnp.where(jnp.logical_and(sends_edge, sends_x), 1, 0)
    )

    @pl.when(jnp.logical_not(has_x))
    def _():
        r_x[...] = jnp.zeros_like(r_x)

    @pl.when(jnp.logical_not(has_edge))
    def _():
        r_edge[...] = jnp.zeros_like(r_edge)

    @pl.when(jnp.logical_not(jnp.logical_and(has_x, has_edge)))
    def _():
        r_corner[...] = jnp.zeros_like(r_corner)

    row = iota((ROWS, 1), 0)
    a_of = jnp.where(row < 24, lax.rem(row, 8), 8)
    b_of = jnp.where(row < 24, row // 8, row - 24)
    valid = row < 27
    pick_first = jnp.where(iota((256, 256), 0) == 32 * gx + iota((256, 256), 1) // 8, 1.0, 0.0).astype(bf16)
    pick_cell = iota((128, 256), 0) - lax.rem(iota((128, 256), 1), 8)
    for n in range(4):
        smalls[n].wait()
    issue(2)
    e_first = jnp.concatenate([ef_v[0:1, :], ef_v[1:2, :]], axis=1)
    o_first = jnp.concatenate([of_v[0:1, :], of_v[1:2, :]], axis=1)
    node_first = 8 * gx + a_of
    sum_first = jnp.sum(raw_weights(e_first, o_first, node_first), axis=1, keepdims=True)
    ex, ox = spread(e_first, o_first, pick_first)
    wide_first = raw_weights(ex, ox, node_first.astype(f32))
    e_third, o_third = et_v[...], ot_v[...]
    for j in range(BLOCKS):
        node_third = 8 * gz + 2 * blocks[j] + b_of
        sum_third = jnp.sum(raw_weights(e_third, o_third, node_third), axis=1, keepdims=True)
        pick = jnp.where(pick_cell == 32 * gz + 8 * blocks[j], 1.0, 0.0).astype(bf16)
        ex, ox = spread(e_third, o_third, pick)
        scale = jnp.where(valid, 1.0 / jnp.where(valid, sum_first * sum_third, 1.0), 0.0)
        wide = wide_first * raw_weights(ex, ox, node_third.astype(f32)) * scale
        high, low = split(wide)
        w1[j, 0:ROWS] = high
        w1[j, ROWS:] = low

    issue(3)
    smalls[4].wait()
    smalls[5].wait()

    def second_weights():
        node_row = iota((40, 1), 0)
        node_second = 32 * gy + node_row
        inside = jnp.logical_and(node_row < 33, node_second < 128)
        total = jnp.zeros((40, 1), f32)
        for n in range(4):
            total += jnp.sum(
                raw_weights(es_v[n : n + 1, :], os_v[n : n + 1, :], node_second), axis=1, keepdims=True
            )
        own = raw_weights(es_v[pl.ds(gy, 1), :], os_v[pl.ds(gy, 1), :], node_second)
        own = jnp.where(inside, own / jnp.where(inside, total, 1.0), 0.0)
        lane_w = iota((128, 128), 1)
        turned = jnp.transpose(jnp.concatenate([own[0:32]] * 4, axis=0))
        turned_edge = jnp.transpose(jnp.broadcast_to(own[32:33], (128, 128)))
        for k in range(4):
            group = lax.rem(gy + k, 4)
            edge_group = lax.rem(gy + 1 + k, 4)
            wide = jnp.concatenate(
                [
                    jnp.where(lane_w // 32 == group, turned, 0.0),
                    jnp.where(lane_w // 32 == edge_group, turned_edge, 0.0),
                ],
                axis=1,
            )
            high, low = split(wide)
            w2h[128 * k : 128 * (k + 1), :] = high
            w2l[128 * k : 128 * (k + 1), :] = low

    def remote(src, dst, send_sem, recv_sem, x, y, z):
        rows = {72: MAIN, 40: EDGE, 16: CROSS, 8: CORNER}[src.shape[0]]
        return pltpu.make_async_remote_copy(
            src_ref=src.at[pl.ds(0, rows)], dst_ref=dst.at[pl.ds(0, rows)], send_sem=send_sem, recv_sem=recv_sem,
            device_id={"gx": x, "gy": y, "gz": z}, device_id_type=MESH,
        )

    sub8 = iota((8, 128), 0)

    def first_stage(j, f):
        slot = (2 * j + f) % 2
        for n in range(2):
            u = 2 * f + n
            for pair in range(2):
                x = jnp.concatenate(
                    [x_buf[j, u, 2 * pair + m].reshape(256, 128) for m in range(2)], axis=1
                )
                high, low = split(x)
                twice = dot(w1[j], high)
                y = twice[0:ROWS] + twice[ROWS:] + dot(w1[j, 0:ROWS], low)
                high, low = split(y)
                columns = slice(256 * pair, 256 * (pair + 1))
                y_buf[slot, ROWS * n : ROWS * (n + 1), columns] = high
                y_buf[slot, ROWS * (2 + n) : ROWS * (3 + n), columns] = low

    sub_wide = iota((8, 256), 0)
    within = lax.rem(iota((8, 128), 1), 32)

    def chosen(where, value):
        return jnp.where(where, value[:, 128:256], 0.0)

    def finish(j, u, rows):
        parts = [rows[8 * n : 8 * (n + 1)] for n in range(4)]
        if blocks[j] > 0 and j > 0:
            corner = pltpu.roll(tail[u, 8:16, :], 6, axis=0)
            parts[0] += tail[u, 0:8, :]
            parts[3] += jnp.where(sub_wide == 0, corner, 0.0)
        if j < BLOCKS - 1:
            tail[u, 0:8, :] = parts[2]
            tail[u, 8:16, :] = parts[3]
        s_main[j, 16 * u : 16 * u + 8, :] = parts[0][:, 0:128]
        s_main[j, 16 * u + 8 : 16 * u + 16, :] = parts[1][:, 0:128]
        s_x[j, 2 * u : 2 * (u + 1), :] = parts[3][0:2, 0:128]
        if j in (0, BLOCKS - 1):
            slot = 0 if j == 0 else 1
            s_edge[slot, 8 * u : 8 * (u + 1), :] = parts[2][:, 0:128]
            s_corner[slot, u : u + 1, :] = parts[3][2:3, 0:128]
        first = 16 * (u % 2)
        main = chosen(within == first + 15 - sub8, parts[0]) + chosen(within == first + 7 - sub8, parts[1])
        cross = chosen(jnp.logical_and(sub8 < 2, within == 7 - 2 * u - sub8), parts[3])
        edge = chosen(within == 8 * u + 7 - sub8, parts[2])
        corner = chosen(jnp.logical_and(sub8 == 2, within == u), parts[3])
        return main, cross, edge, corner

    def second_stage(j, f):
        y = y_buf[(2 * j + f) % 2]
        twice = dot(y, w2h[...])
        n = 2 * ROWS
        z = twice[0:n] + twice[n:] + dot(y[0:n], w2l[...])
        sums = [
            a + b
            for a, b in zip(finish(j, 2 * f, z[0:ROWS]), finish(j, 2 * f + 1, z[ROWS:]))
        ]

        def row_of(value):
            return jnp.sum(value, axis=0, keepdims=True)

        s_main[j, 16 * CHUNKS + f : 16 * CHUNKS + f + 1, :] = row_of(sums[0])
        if f == 0:
            for n in range(3):
                extra_buf[8 * n : 8 * (n + 1), :] = sums[n + 1]
        else:
            rest = [row_of(sums[n + 1] + extra_buf[8 * n : 8 * (n + 1), :]) for n in range(3)]
            s_x[j, CROSS - 1 : CROSS, :] = rest[0]
            if j in (0, BLOCKS - 1):
                slot = 0 if j == 0 else 1
                s_edge[slot, EDGE - 1 : EDGE, :] = rest[1]
                s_corner[slot, CORNER - 1 : CORNER, :] = rest[2]

    both = jnp.logical_and
    copies = {}
    for j, block in enumerate(blocks):
        copies["x", j] = (sends_x, remote(
            s_x.at[j], r_x.at[gy], ss_x.at[j], rs_x.at[gy], gx + 1, gz, block))
        if j == 0:
            copies["corner", 0] = (both(sends_edge, sends_x), remote(
                s_corner.at[0], r_corner.at[gy], ss_corner.at[0], rs_corner.at[gy],
                gx + 1, gz + 1, 0))
            copies["edge", 0] = (both(sends_edge, jnp.logical_not(edge_self)), remote(
                s_edge.at[0], r_edge.at[gy], ss_edge.at[0], rs_edge.at[gy], gx, gz + 1, 0))
        copies["main", j] = (jnp.logical_not(both(gy == gz, gz == block)), remote(
            s_main.at[j], r_main.at[gy], ss_main.at[j], rs_main.at[gy], gx, gz, block))
        if j == BLOCKS - 1:
            copies["corner", 1] = (sends_x, remote(
                s_corner.at[1], r_corner.at[gy], ss_corner.at[1], rs_corner.at[gy],
                gx + 1, gz, BLOCKS - 1))
            copies["edge", 1] = (jnp.logical_not(last_self), remote(
                s_edge.at[1], r_edge.at[gy], ss_edge.at[1], rs_edge.at[gy],
                gx, gz, BLOCKS - 1))

    READY = [
        [("corner", 0), ("edge", 0), ("main", 0)],
        [("x", 1), ("main", 1)],
        [("x", 2), ("main", 2)],
        [("main", 3), ("edge", 1)],
    ]
    RANK = {name: n for n, name in enumerate((("x", 1), ("corner", 0), ("main", 1), ("edge", 0), ("main", 0), ("x", 2), ("main", 2), ("main", 3), ("edge", 1)))}

    def send(names, when=None):
        for name in names:
            condition, copy = copies[name]
            condition = condition if when is None else both(condition, when)

            @pl.when(condition)
            def _():
                copy.start()

    def enter(when):
        @pl.when(when)
        def _():
            pl.semaphore_wait(barrier, expected)

        for c in range(4):
            @pl.when(both(both(when, relays), jnp.logical_not(main_self(c))))
            def _():
                pl.semaphore_signal(
                    x_ready.at[lax.max(gz - 2, 0)], inc=1,
                    device_id={"gx": gx, "gy": c, "gz": gy}, device_id_type=MESH,
                )

        @pl.when(both(both(when, relays), gy == gz))
        def _():
            pl.semaphore_signal(x_ready.at[lax.max(gz - 2, 0)], inc=1)

    place = jnp.where(gx == 3, jnp.where(gz == 2, PLACE[5], PLACE[4]), jnp.where(
        gz == 0, PLACE[0], jnp.where(gz == 1, PLACE[1], jnp.where(gz == 2, PLACE[2], PLACE[3]))))
    for h in range(2 * BLOCKS + 1):
        j, f = h // 2, h % 2
        if h < 2 * BLOCKS:
            for u in range(2 * f, 2 * f + 2):
                loads[j, u].wait()
        if h == 0:
            second_weights()
        else:
            second_stage((h - 1) // 2, (h - 1) % 2)
        if h < 2 * BLOCKS:
            first_stage(j, f)
        if h in PLACE:
            here = place == h
            enter(here)
            names = [name for i in range(j) for name in READY[i]]
            send(sorted(names, key=lambda name: RANK[name]), here)
        if h > min(PLACE) and f == 0:
            send(READY[j - 1], place < h)

    for n, names in ((1, [("x", 0), ("corner", 1)]), (0, [("x", 3)])):
        @pl.when(sends_x)
        def _():
            pl.semaphore_wait(x_ready.at[n], 1)

        send(names)

    for j, block in enumerate(blocks):
        @pl.when(both(gy == gz, gz == block))
        def _():
            r_main[pl.ds(gy, 1)] = s_main[j : j + 1]

    @pl.when(both(sends_edge, edge_self))
    def _():
        r_edge[pl.ds(gy, 1)] = s_edge[0:1]

    @pl.when(last_self)
    def _():
        r_edge[pl.ds(gy, 1)] = s_edge[1:2]

    def arrive(when, buf, sems, c, source):
        @pl.when(when)
        def _():
            remote(source, buf.at[c], ss_main.at[0], sems.at[c], gx, gy, gz).wait_recv()

    for c in range(4):
        arrive(jnp.logical_not(main_self(c)), r_main, rs_main, c, s_main.at[0])
        arrive(jnp.logical_and(has_edge, jnp.logical_not(jnp.logical_or(below_self(c), both(last_self, gy == c)))), r_edge, rs_edge, c, s_edge.at[0])
        arrive(has_x, r_x, rs_x, c, s_x.at[0])
        arrive(jnp.logical_and(has_x, has_edge), r_corner, rs_corner, c, s_corner.at[0])
    for n in range(6, 10):
        smalls[n].wait()

    top = sub8 == 0
    lane = iota((8, 128), 1)
    group = lane // 32
    lead = lax.rem(lane, 32) == 0

    def gathered(c, u):
        low_rows = (
            r_main[c, 16 * u : 16 * u + 8, :]
            + r_edge[c, 8 * u : 8 * u + 8, :]
            + jnp.where(top, r_x[c, 2 * u : 2 * u + 1, :] + r_corner[c, u : u + 1, :], 0.0)
        )
        high_rows = r_main[c, 16 * u + 8 : 16 * u + 16, :] + jnp.where(
            top, r_x[c, 2 * u + 1 : 2 * u + 2, :], 0.0
        )
        return low_rows, high_rows

    def unpicked(row, shift):
        return pltpu.roll(
            jnp.broadcast_to(row, (8, 128)), shift % 128, axis=1, stride=1, stride_axis=0
        )

    crosses = [unpicked(r_x[c, CROSS - 1 : CROSS, :], 121) for c in range(4)]

    def edges_of(c, u):
        row = 16 * CHUNKS + u // 2
        row = r_main[c, row : row + 1, :]
        corner = r_corner[c, CORNER - 1 : CORNER, :]
        corner = pltpu.roll(corner, 128 - u, axis=1) if u else corner
        cross = crosses[c]
        low_rows = (
            unpicked(row, 113 - 16 * (u % 2))
            + unpicked(r_edge[c, EDGE - 1 : EDGE, :], 121 - 8 * u)
            + jnp.where(top, cross[2 * u : 2 * u + 1] + corner, 0.0)
        )
        high_rows = unpicked(row, 121 - 16 * (u % 2)) + jnp.where(
            top, cross[2 * u + 1 : 2 * u + 2], 0.0
        )
        return low_rows, high_rows

    def by_group(values, shift):
        out = values[(0 - shift) % 4]
        for h in range(1, 4):
            out = jnp.where(group == h, values[(h - shift) % 4], out)
        return out

    drive = {}
    for u in range(CHUNKS):
        mains = [gathered(c, u) for c in range(4)]
        picked = [edges_of(c, u) for c in range(4)]
        for b in range(2):
            edges = [jnp.where(lead, picked[c][b], 0.0) for c in range(4)]
            for k in range(4):
                value = by_group([mains[c][b] for c in range(4)], k) + by_group(edges, k + 1)
                if k:
                    value = pltpu.roll(value, 128 - 32 * k, axis=1)
                drive[u // 2, 4 * (u % 2) + k, b] = value

    for b in range(2):
        bound, active = trop_v[:, b, :], tens_v[:, b, :]
        unbind, relax = unb_v[:, b, :], rel_v[:, b, :]
        keep_bound = 1.0 - step_size * unbind
        keep_active = 1.0 - step_size * relax
        for t in range(8):
            squared = drive[0, t, b] * drive[0, t, b]
            gain = (step_size * bind_rate) * (squared / (squared + half_square))
            pull = (step_size * peak_tension) * relax * drive[1, t, b]
            bound = bound * (keep_bound - gain) + gain
            active = active * keep_active + pull * bound
        out_bound[:, b, :] = bound
        out_active[:, b, :] = active

    for when, copy in copies.values():
        @pl.when(when)
        def _():
            copy.wait_send()


def write_out(bound, active, out_bound, out_active, sems):
    copies = [
        pltpu.make_async_copy(bound, out_bound, sems.at[0]),
        pltpu.make_async_copy(active, out_active, sems.at[1]),
    ]
    for copy in copies:
        copy.start()
    for copy in copies:
        copy.wait()


def per_device(
    calcium, activation,
    element_first, offset_first, element_second, offset_second, element_third, offset_third,
    troponin, tension, unbind_rate, relax_rate,
):
    anywhere = pl.BlockSpec(memory_space=pltpu.HBM)
    vmem = pl.BlockSpec(memory_space=pltpu.VMEM)
    dma = pltpu.SemaphoreType.DMA
    small = jax.ShapeDtypeStruct(troponin.shape, f32)
    kept = pltpu.VMEM(troponin.shape, f32)
    bound, active = pl.pallas_call(
        kernel,
        out_shape=(kept, kept),
        in_specs=[anywhere] * 12,
        out_specs=(vmem, vmem),
        scratch_shapes=[
            pltpu.VMEM((BLOCKS, CHUNKS, 4, 32, 8, 128), f32),
            pltpu.VMEM((2, 128), jnp.int32),
            pltpu.VMEM((2, 128), f32),
            pltpu.VMEM((4, 128), jnp.int32),
            pltpu.VMEM((4, 128), f32),
            pltpu.VMEM((1, 128), jnp.int32),
            pltpu.VMEM((1, 128), f32),
            *[pltpu.VMEM(troponin.shape, f32) for _ in range(4)],
            pltpu.VMEM((BLOCKS, 2 * ROWS, 256), bf16),
            pltpu.VMEM((512, 256), bf16),
            pltpu.VMEM((512, 256), bf16),
            pltpu.VMEM((2, 4 * ROWS, 512), bf16),
            pltpu.VMEM((CHUNKS, 16, 256), f32),
            pltpu.VMEM((24, 128), f32),
            pltpu.VMEM((BLOCKS, 72, 128), f32),
            pltpu.VMEM((BLOCKS, 16, 128), f32),
            pltpu.VMEM((2, 40, 128), f32),
            pltpu.VMEM((2, 8, 128), f32),
            pltpu.VMEM((4, 72, 128), f32),
            pltpu.VMEM((4, 16, 128), f32),
            pltpu.VMEM((4, 40, 128), f32),
            pltpu.VMEM((4, 8, 128), f32),
            dma((BLOCKS, CHUNKS)),
            dma((10,)),
            dma((BLOCKS,)),
            dma((BLOCKS,)),
            dma((2,)),
            dma((2,)),
            dma((4,)),
            dma((4,)),
            dma((4,)),
            dma((4,)),
            pltpu.SemaphoreType.REGULAR((2,)),
        ],
        compiler_params=pltpu.CompilerParams(
            collective_id=0, has_side_effects=True, vmem_limit_bytes=60 * 1024 * 1024
        ),
        name="restrict_and_step",
    )(
        calcium, activation,
        element_first.reshape(2, 128), offset_first.reshape(2, 128),
        element_second.reshape(4, 128), offset_second.reshape(4, 128),
        element_third.reshape(1, 128), offset_third.reshape(1, 128),
        troponin, tension, unbind_rate, relax_rate,
    )
    return pl.pallas_call(
        write_out,
        out_shape=(small, small),
        in_specs=[vmem, vmem],
        out_specs=(anywhere, anywhere),
        scratch_shapes=[dma((2,))],
        compiler_params=pltpu.CompilerParams(vmem_limit_bytes=2**20),
        name="write_out",
    )(bound, active)


def solution(mesh):
    nodes = P("gx", ("gy", "gz"), None)
    fine = P(None, "gx", "gz", "gy")
    return jax.shard_map(
        per_device,
        mesh=mesh,
        in_specs=(fine, fine, P(), P(), P(), P(), P(), P(), nodes, nodes, nodes, nodes),
        out_specs=(nodes, nodes),
        check_vma=False,
    )
```

```python
import functools

import jax
import jax.numpy as jnp
from jax import lax
from jax.experimental import pallas as pl
from jax.experimental.pallas import tpu as pltpu
from jax.sharding import PartitionSpec as P

step_size = 0.2
bind_rate = 2.0
peak_tension = 2.0
half_square = 0.25
MESH = pl.DeviceIdType.MESH
f32 = jnp.float32
bf16 = jnp.bfloat16

SLABS = 4
BLOCKS = 4
ROWS = 32
CHUNKS = 4
ORDER = (0, 3, 1, 2)
PLACE = (4, 4, 2, 2, 4, 4, 3, 3)
MAIN = CHUNKS * 16 + 2
EDGE = CHUNKS * 8 + 1
CROSS = CHUNKS * 2 + 1
CORNER = CHUNKS + 1


def raw_weights(element, offset, node):
    return jnp.where(element == node, 1.0 - offset, 0.0) + jnp.where(
        element + 1 == node, offset, 0.0
    )


def split(x):
    high = x.astype(bf16)
    low = (x - high.astype(f32)).astype(bf16)
    return high, low


def dot(a, b):
    return jnp.dot(a, b, preferred_element_type=f32)


def iota(shape, dim):
    return lax.broadcasted_iota(jnp.int32, shape, dim)


def spread(element, offset, pick):
    cells = element.shape[1]
    first = offset.astype(bf16).astype(f32)
    second = (offset - first).astype(bf16).astype(f32)
    third = offset - first - second
    row = iota((16, cells), 0)
    stack = jnp.where(
        row == 0,
        element.astype(f32),
        jnp.where(row == 1, first, jnp.where(row == 2, second, jnp.where(row == 3, third, 0.0))),
    )
    out = dot(stack.astype(bf16), pick)
    return out[0:1], out[1:2] + out[2:3] + out[3:4]


def kernel(
    cal, act, ef, of, es, os_, et, ot, trop, tens, unb, rel,
    out_bound, out_active,
    x_buf, ef_v, of_v, es_v, os_v, et_v, ot_v, trop_v, tens_v, unb_v, rel_v,
    w1, w2h, w2l, y_buf, tail, extra_buf,
    s_main, s_x, s_edge, s_corner,
    r_main, r_x, r_edge, r_corner,
    sem_x, sem_small,
    ss_main, ss_x, ss_edge, ss_corner,
    rs_main, rs_x, rs_edge, rs_corner, x_ready,
):
    gx, gy, gz = lax.axis_index("gx"), lax.axis_index("gy"), lax.axis_index("gz")
    last_x = lax.axis_size("gx") - 1
    blocks = ORDER

    smalls = [
        pltpu.make_async_copy(src, dst, sem_small.at[n])
        for n, (src, dst) in enumerate(
            [(ef, ef_v), (of, of_v), (et, et_v), (ot, ot_v), (es, es_v), (os_, os_v),
             (trop, trop_v), (tens, tens_v), (unb, unb_v), (rel, rel_v)]
        )
    ]
    barrier = pltpu.get_barrier_semaphore()

    def ready(x, y, z):
        pl.semaphore_signal(
            barrier, inc=1, device_id={"gx": x, "gy": y, "gz": z}, device_id_type=MESH
        )

    from_below = jnp.logical_and(gz == 0, gy > 0)
    has_edge = jnp.logical_or(from_below, gz == SLABS - 1)
    has_x = gx > 0
    sends_x = gx < last_x
    sends_edge = gz < SLABS - 1

    near = gz < 2
    relays = jnp.logical_and(gz >= 2, sends_x)

    for c in range(4):
        @pl.when(jnp.logical_and(has_x, near))
        def _():
            ready(gx - 1, c, gy)

        @pl.when(jnp.logical_and(has_x, from_below))
        def _():
            ready(gx - 1, c, gy - 1)

    @pl.when(jnp.logical_and(has_x, gz >= 2))
    def _():
        ready(gx - 1, gy, gz)

    for q in (2, 3):
        @pl.when(jnp.logical_and(sends_x, jnp.logical_not(jnp.logical_and(gy == gz, gz == q))))
        def _():
            ready(gx, gz, q)

    for copy in smalls[:6]:
        copy.start()

    @pl.when(jnp.logical_or(gy != gz, gy != 0))
    def _():
        ready(gx, 0, gy)

    loads = {}
    for j in range(BLOCKS):
        first_cell = blocks[j] * 8
        for u in range(CHUNKS):
            src = (cal, act)[u // 2].at[pl.ds(4 * (u % 2), 4), :, pl.ds(first_cell, 8), :]
            loads[j, u] = pltpu.make_async_copy(src, x_buf.at[j, u], sem_x.at[j, u])

    def issue(j):
        for u in range(CHUNKS):
            loads[j, u].start()

    issue(0)
    for copy in smalls[6:]:
        copy.start()

    def main_self(c):
        return jnp.logical_and(gy == gz, gy == c)

    def below_self(c):
        return jnp.logical_and(jnp.logical_and(gy == 1, gz == 0), gy == c)

    last_self = jnp.logical_and(gy == SLABS - 1, gz == SLABS - 1)

    for c in range(4):
        if c > 0:
            @pl.when(jnp.logical_not(main_self(c)))
            def _():
                ready(gx, c, gy)

        @pl.when(jnp.logical_and(from_below, jnp.logical_not(below_self(c))))
        def _():
            ready(gx, c, gy - 1)

    issue(1)
    edge_self = jnp.logical_and(gz == 0, gy == 1)
    expected = (
        jnp.where(gy == gz, 3, 4)
        + jnp.where(sends_x, 2, 0)
        + jnp.where(relays, jnp.where(gy == gz, 4, 5), 0)
        + jnp.where(jnp.logical_and(sends_edge, jnp.logical_not(edge_self)), 1, 0)
        + jnp.where(jnp.logical_and(sends_edge, sends_x), 1, 0)
    )

    @pl.when(jnp.logical_not(has_x))
    def _():
        r_x[...] = jnp.zeros_like(r_x)

    @pl.when(jnp.logical_not(has_edge))
    def _():
        r_edge[...] = jnp.zeros_like(r_edge)

    @pl.when(jnp.logical_not(jnp.logical_and(has_x, has_edge)))
    def _():
        r_corner[...] = jnp.zeros_like(r_corner)

    row = iota((ROWS, 1), 0)
    a_of = jnp.where(row < 24, lax.rem(row, 8), 8)
    b_of = jnp.where(row < 24, row // 8, row - 24)
    valid = row < 27
    pick_first = jnp.where(iota((256, 256), 0) == 32 * gx + iota((256, 256), 1) // 8, 1.0, 0.0).astype(bf16)
    pick_cell = iota((128, 256), 0) - lax.rem(iota((128, 256), 1), 8)
    for n in range(4):
        smalls[n].wait()
    issue(2)
    e_first = jnp.concatenate([ef_v[0:1, :], ef_v[1:2, :]], axis=1)
    o_first = jnp.concatenate([of_v[0:1, :], of_v[1:2, :]], axis=1)
    node_first = 8 * gx + a_of
    sum_first = jnp.sum(raw_weights(e_first, o_first, node_first), axis=1, keepdims=True)
    ex, ox = spread(e_first, o_first, pick_first)
    wide_first = raw_weights(ex, ox, node_first.astype(f32))
    e_third, o_third = et_v[...], ot_v[...]
    for j in range(BLOCKS):
        node_third = 8 * gz + 2 * blocks[j] + b_of
        sum_third = jnp.sum(raw_weights(e_third, o_third, node_third), axis=1, keepdims=True)
        pick = jnp.where(pick_cell == 32 * gz + 8 * blocks[j], 1.0, 0.0).astype(bf16)
        ex, ox = spread(e_third, o_third, pick)
        scale = jnp.where(valid, 1.0 / jnp.where(valid, sum_first * sum_third, 1.0), 0.0)
        wide = wide_first * raw_weights(ex, ox, node_third.astype(f32)) * scale
        high, low = split(wide)
        w1[j, 0:ROWS] = high
        w1[j, ROWS:] = low

    issue(3)
    smalls[4].wait()
    smalls[5].wait()

    def second_weights():
        node_row = iota((40, 1), 0)
        node_second = 32 * gy + node_row
        inside = jnp.logical_and(node_row < 33, node_second < 128)
        total = jnp.zeros((40, 1), f32)
        for n in range(4):
            total += jnp.sum(
                raw_weights(es_v[n : n + 1, :], os_v[n : n + 1, :], node_second), axis=1, keepdims=True
            )
        own = raw_weights(es_v[pl.ds(gy, 1), :], os_v[pl.ds(gy, 1), :], node_second)
        own = jnp.where(inside, own / jnp.where(inside, total, 1.0), 0.0)
        lane_w = iota((128, 128), 1)
        turned = jnp.transpose(jnp.concatenate([own[0:32]] * 4, axis=0))
        turned_edge = jnp.transpose(jnp.broadcast_to(own[32:33], (128, 128)))
        for k in range(4):
            group = lax.rem(gy + k, 4)
            edge_group = lax.rem(gy + 1 + k, 4)
            wide = jnp.concatenate(
                [
                    jnp.where(lane_w // 32 == group, turned, 0.0),
                    jnp.where(lane_w // 32 == edge_group, turned_edge, 0.0),
                ],
                axis=1,
            )
            high, low = split(wide)
            w2h[128 * k : 128 * (k + 1), :] = high
            w2l[128 * k : 128 * (k + 1), :] = low

    def remote(src, dst, send_sem, recv_sem, x, y, z):
        rows = {72: MAIN, 40: EDGE, 16: CROSS, 8: CORNER}[src.shape[0]]
        return pltpu.make_async_remote_copy(
            src_ref=src.at[pl.ds(0, rows)], dst_ref=dst.at[pl.ds(0, rows)], send_sem=send_sem, recv_sem=recv_sem,
            device_id={"gx": x, "gy": y, "gz": z}, device_id_type=MESH,
        )

    sub8 = iota((8, 128), 0)

    def first_stage(j, f):
        slot = (2 * j + f) % 2
        for n in range(2):
            u = 2 * f + n
            for pair in range(2):
                x = jnp.concatenate(
                    [x_buf[j, u, 2 * pair + m].reshape(256, 128) for m in range(2)], axis=1
                )
                high, low = split(x)
                twice = dot(w1[j], high)
                y = twice[0:ROWS] + twice[ROWS:] + dot(w1[j, 0:ROWS], low)
                high, low = split(y)
                columns = slice(256 * pair, 256 * (pair + 1))
                y_buf[slot, ROWS * n : ROWS * (n + 1), columns] = high
                y_buf[slot, ROWS * (2 + n) : ROWS * (3 + n), columns] = low

    sub_wide = iota((8, 256), 0)
    within = lax.rem(iota((8, 128), 1), 32)

    def chosen(where, value):
        return jnp.where(where, value[:, 128:256], 0.0)

    def finish(j, u, rows):
        parts = [rows[8 * n : 8 * (n + 1)] for n in range(4)]
        if blocks[j] in (1, 2):
            corner = pltpu.roll(tail[u, 8:16, :], 6, axis=0)
            parts[0] += tail[u, 0:8, :]
            parts[3] += jnp.where(sub_wide == 0, corner, 0.0)
        if blocks[j] in (0, 1):
            tail[u, 0:8, :] = parts[2]
            tail[u, 8:16, :] = parts[3]
        s_main[j, 16 * u : 16 * u + 8, :] = parts[0][:, 0:128]
        s_main[j, 16 * u + 8 : 16 * u + 16, :] = parts[1][:, 0:128]
        s_x[j, 2 * u : 2 * (u + 1), :] = parts[3][0:2, 0:128]
        if blocks[j] in (2, 3):
            slot = 3 - blocks[j]
            s_edge[slot, 8 * u : 8 * (u + 1), :] = parts[2][:, 0:128]
            s_corner[slot, u : u + 1, :] = parts[3][2:3, 0:128]
        first = 16 * (u % 2)
        main = chosen(within == first + 15 - sub8, parts[0]) + chosen(within == first + 7 - sub8, parts[1])
        cross = chosen(jnp.logical_and(sub8 < 2, within == 7 - 2 * u - sub8), parts[3])
        edge = chosen(within == 8 * u + 7 - sub8, parts[2])
        corner = chosen(jnp.logical_and(sub8 == 2, within == u), parts[3])
        return main, cross, edge, corner

    def second_stage(j, f):
        y = y_buf[(2 * j + f) % 2]
        twice = dot(y, w2h[...])
        n = 2 * ROWS
        z = twice[0:n] + twice[n:] + dot(y[0:n], w2l[...])
        sums = [
            a + b
            for a, b in zip(finish(j, 2 * f, z[0:ROWS]), finish(j, 2 * f + 1, z[ROWS:]))
        ]

        def row_of(value):
            return jnp.sum(value, axis=0, keepdims=True)

        s_main[j, 16 * CHUNKS + f : 16 * CHUNKS + f + 1, :] = row_of(sums[0])
        if f == 0:
            for n in range(3):
                extra_buf[8 * n : 8 * (n + 1), :] = sums[n + 1]
        else:
            rest = [row_of(sums[n + 1] + extra_buf[8 * n : 8 * (n + 1), :]) for n in range(3)]
            s_x[j, CROSS - 1 : CROSS, :] = rest[0]
            if blocks[j] in (2, 3):
                slot = 3 - blocks[j]
                s_edge[slot, EDGE - 1 : EDGE, :] = rest[1]
                s_corner[slot, CORNER - 1 : CORNER, :] = rest[2]

    both = jnp.logical_and
    copies = {}
    for j, block in enumerate(blocks):
        copies["x", j] = (sends_x, remote(
            s_x.at[j], r_x.at[gy], ss_x.at[j], rs_x.at[gy], gx + 1, gz, block))
        if block == BLOCKS - 1:
            copies["corner", 0] = (both(sends_edge, sends_x), remote(
                s_corner.at[0], r_corner.at[gy], ss_corner.at[0], rs_corner.at[gy],
                gx + 1, gz + 1, 0))
            copies["edge", 0] = (both(sends_edge, jnp.logical_not(edge_self)), remote(
                s_edge.at[0], r_edge.at[gy], ss_edge.at[0], rs_edge.at[gy], gx, gz + 1, 0))
        copies["main", j] = (jnp.logical_not(both(gy == gz, gz == block)), remote(
            s_main.at[j], r_main.at[gy], ss_main.at[j], rs_main.at[gy], gx, gz, block))
        if j == BLOCKS - 1:
            copies["corner", 1] = (sends_x, remote(
                s_corner.at[1], r_corner.at[gy], ss_corner.at[1], rs_corner.at[gy],
                gx + 1, gz, BLOCKS - 1))
            copies["edge", 1] = (jnp.logical_not(last_self), remote(
                s_edge.at[1], r_edge.at[gy], ss_edge.at[1], rs_edge.at[gy],
                gx, gz, BLOCKS - 1))

    READY = [
        [("x", 0), ("main", 0)],
        [("corner", 0), ("edge", 0), ("main", 1)],
        [("x", 2), ("main", 2)],
        [("main", 3), ("edge", 1)],
    ]
    RANK = {name: n for n, name in enumerate((
        ("x", 0), ("corner", 0), ("main", 0), ("edge", 0), ("main", 1),
        ("x", 2), ("main", 2), ("main", 3), ("edge", 1)))}

    def send(names, when=None):
        for name in names:
            condition, copy = copies[name]
            condition = condition if when is None else both(condition, when)

            @pl.when(condition)
            def _():
                copy.start()

    def enter(when):
        @pl.when(when)
        def _():
            pl.semaphore_wait(barrier, expected)

        for c in range(4):
            @pl.when(both(both(when, relays), jnp.logical_not(main_self(c))))
            def _():
                pl.semaphore_signal(
                    x_ready.at[lax.max(gz - 2, 0)], inc=1,
                    device_id={"gx": gx, "gy": c, "gz": gy}, device_id_type=MESH,
                )

        @pl.when(both(both(when, relays), gy == gz))
        def _():
            pl.semaphore_signal(x_ready.at[lax.max(gz - 2, 0)], inc=1)

    def by_gz(values):
        out = values[3]
        for n in range(3):
            out = jnp.where(gz == n, values[n], out)
        return out

    place = jnp.where(gx == 3, by_gz(PLACE[4:]), by_gz(PLACE[:4]))
    for h in range(2 * BLOCKS + 1):
        j, f = h // 2, h % 2
        if h < 2 * BLOCKS:
            for u in range(2 * f, 2 * f + 2):
                loads[j, u].wait()
        if h == 0:
            second_weights()
        else:
            second_stage((h - 1) // 2, (h - 1) % 2)
        if h < 2 * BLOCKS:
            first_stage(j, f)
        if h in PLACE:
            here = place == h
            enter(here)
            names = [name for i in range(j) for name in READY[i]]
            send(sorted(names, key=lambda name: RANK[name]), here)
        if h > min(PLACE) and f == 0:
            send(READY[j - 1], place < h)

    for n, names in ((1, [("x", 1), ("corner", 1)]), (0, [("x", 3)])):
        @pl.when(sends_x)
        def _():
            pl.semaphore_wait(x_ready.at[n], 1)

        send(names)

    for j, block in enumerate(blocks):
        @pl.when(both(gy == gz, gz == block))
        def _():
            r_main[pl.ds(gy, 1)] = s_main[j : j + 1]

    @pl.when(both(sends_edge, edge_self))
    def _():
        r_edge[pl.ds(gy, 1)] = s_edge[0:1]

    @pl.when(last_self)
    def _():
        r_edge[pl.ds(gy, 1)] = s_edge[1:2]

    def arrive(when, buf, sems, c, source):
        @pl.when(when)
        def _():
            remote(source, buf.at[c], ss_main.at[0], sems.at[c], gx, gy, gz).wait_recv()

    for c in range(4):
        arrive(jnp.logical_not(main_self(c)), r_main, rs_main, c, s_main.at[0])
        arrive(jnp.logical_and(has_edge, jnp.logical_not(jnp.logical_or(below_self(c), both(last_self, gy == c)))), r_edge, rs_edge, c, s_edge.at[0])
        arrive(has_x, r_x, rs_x, c, s_x.at[0])
        arrive(jnp.logical_and(has_x, has_edge), r_corner, rs_corner, c, s_corner.at[0])
    for n in range(6, 10):
        smalls[n].wait()

    top = sub8 == 0
    lane = iota((8, 128), 1)
    group = lane // 32
    lead = lax.rem(lane, 32) == 0

    def gathered(c, u):
        low_rows = (
            r_main[c, 16 * u : 16 * u + 8, :]
            + r_edge[c, 8 * u : 8 * u + 8, :]
            + jnp.where(top, r_x[c, 2 * u : 2 * u + 1, :] + r_corner[c, u : u + 1, :], 0.0)
        )
        high_rows = r_main[c, 16 * u + 8 : 16 * u + 16, :] + jnp.where(
            top, r_x[c, 2 * u + 1 : 2 * u + 2, :], 0.0
        )
        return low_rows, high_rows

    def unpicked(row, shift):
        return pltpu.roll(
            jnp.broadcast_to(row, (8, 128)), shift % 128, axis=1, stride=1, stride_axis=0
        )

    crosses = [unpicked(r_x[c, CROSS - 1 : CROSS, :], 121) for c in range(4)]

    def edges_of(c, u):
        row = 16 * CHUNKS + u // 2
        row = r_main[c, row : row + 1, :]
        corner = r_corner[c, CORNER - 1 : CORNER, :]
        corner = pltpu.roll(corner, 128 - u, axis=1) if u else corner
        cross = crosses[c]
        low_rows = (
            unpicked(row, 113 - 16 * (u % 2))
            + unpicked(r_edge[c, EDGE - 1 : EDGE, :], 121 - 8 * u)
            + jnp.where(top, cross[2 * u : 2 * u + 1] + corner, 0.0)
        )
        high_rows = unpicked(row, 121 - 16 * (u % 2)) + jnp.where(
            top, cross[2 * u + 1 : 2 * u + 2], 0.0
        )
        return low_rows, high_rows

    def by_group(values, shift):
        out = values[(0 - shift) % 4]
        for h in range(1, 4):
            out = jnp.where(group == h, values[(h - shift) % 4], out)
        return out

    drive = {}
    for u in range(CHUNKS):
        mains = [gathered(c, u) for c in range(4)]
        picked = [edges_of(c, u) for c in range(4)]
        for b in range(2):
            edges = [jnp.where(lead, picked[c][b], 0.0) for c in range(4)]
            for k in range(4):
                value = by_group([mains[c][b] for c in range(4)], k) + by_group(edges, k + 1)
                if k:
                    value = pltpu.roll(value, 128 - 32 * k, axis=1)
                drive[u // 2, 4 * (u % 2) + k, b] = value

    for b in range(2):
        bound, active = trop_v[:, b, :], tens_v[:, b, :]
        unbind, relax = unb_v[:, b, :], rel_v[:, b, :]
        keep_bound = 1.0 - step_size * unbind
        keep_active = 1.0 - step_size * relax
        for t in range(8):
            squared = drive[0, t, b] * drive[0, t, b]
            gain = (step_size * bind_rate) * (squared / (squared + half_square))
            pull = (step_size * peak_tension) * relax * drive[1, t, b]
            bound = bound * (keep_bound - gain) + gain
            active = active * keep_active + pull * bound
        out_bound[:, b, :] = bound
        out_active[:, b, :] = active

    for when, copy in copies.values():
        @pl.when(when)
        def _():
            copy.wait_send()


def write_out(bound, active, out_bound, out_active, sems):
    copies = [
        pltpu.make_async_copy(bound, out_bound, sems.at[0]),
        pltpu.make_async_copy(active, out_active, sems.at[1]),
    ]
    for copy in copies:
        copy.start()
    for copy in copies:
        copy.wait()


def per_device(
    calcium, activation,
    element_first, offset_first, element_second, offset_second, element_third, offset_third,
    troponin, tension, unbind_rate, relax_rate,
):
    anywhere = pl.BlockSpec(memory_space=pltpu.HBM)
    vmem = pl.BlockSpec(memory_space=pltpu.VMEM)
    dma = pltpu.SemaphoreType.DMA
    small = jax.ShapeDtypeStruct(troponin.shape, f32)
    kept = pltpu.VMEM(troponin.shape, f32)
    bound, active = pl.pallas_call(
        kernel,
        out_shape=(kept, kept),
        in_specs=[anywhere] * 12,
        out_specs=(vmem, vmem),
        scratch_shapes=[
            pltpu.VMEM((BLOCKS, CHUNKS, 4, 32, 8, 128), f32),
            pltpu.VMEM((2, 128), jnp.int32),
            pltpu.VMEM((2, 128), f32),
            pltpu.VMEM((4, 128), jnp.int32),
            pltpu.VMEM((4, 128), f32),
            pltpu.VMEM((1, 128), jnp.int32),
            pltpu.VMEM((1, 128), f32),
            *[pltpu.VMEM(troponin.shape, f32) for _ in range(4)],
            pltpu.VMEM((BLOCKS, 2 * ROWS, 256), bf16),
            pltpu.VMEM((512, 256), bf16),
            pltpu.VMEM((512, 256), bf16),
            pltpu.VMEM((2, 4 * ROWS, 512), bf16),
            pltpu.VMEM((CHUNKS, 16, 256), f32),
            pltpu.VMEM((24, 128), f32),
            pltpu.VMEM((BLOCKS, 72, 128), f32),
            pltpu.VMEM((BLOCKS, 16, 128), f32),
            pltpu.VMEM((2, 40, 128), f32),
            pltpu.VMEM((2, 8, 128), f32),
            pltpu.VMEM((4, 72, 128), f32),
            pltpu.VMEM((4, 16, 128), f32),
            pltpu.VMEM((4, 40, 128), f32),
            pltpu.VMEM((4, 8, 128), f32),
            dma((BLOCKS, CHUNKS)),
            dma((10,)),
            dma((BLOCKS,)),
            dma((BLOCKS,)),
            dma((2,)),
            dma((2,)),
            dma((4,)),
            dma((4,)),
            dma((4,)),
            dma((4,)),
            pltpu.SemaphoreType.REGULAR((2,)),
        ],
        compiler_params=pltpu.CompilerParams(
            collective_id=0, has_side_effects=True, vmem_limit_bytes=60 * 1024 * 1024
        ),
        name="restrict_and_step",
    )(
        calcium, activation,
        element_first.reshape(2, 128), offset_first.reshape(2, 128),
        element_second.reshape(4, 128), offset_second.reshape(4, 128),
        element_third.reshape(1, 128), offset_third.reshape(1, 128),
        troponin, tension, unbind_rate, relax_rate,
    )
    return pl.pallas_call(
        write_out,
        out_shape=(small, small),
        in_specs=[vmem, vmem],
        out_specs=(anywhere, anywhere),
        scratch_shapes=[dma((2,))],
        compiler_params=pltpu.CompilerParams(vmem_limit_bytes=2**20),
        name="write_out",
    )(bound, active)


def solution(mesh):
    nodes = P("gx", ("gy", "gz"), None)
    fine = P(None, "gx", "gz", "gy")
    return jax.shard_map(
        per_device,
        mesh=mesh,
        in_specs=(fine, fine, P(), P(), P(), P(), P(), P(), nodes, nodes, nodes, nodes),
        out_specs=(nodes, nodes),
        check_vma=False,
    )
```

```python
import functools

import jax
import jax.numpy as jnp
from jax import lax
from jax.experimental import pallas as pl
from jax.experimental.pallas import tpu as pltpu
from jax.sharding import PartitionSpec as P

step_size = 0.2
bind_rate = 2.0
peak_tension = 2.0
half_square = 0.25
MESH = pl.DeviceIdType.MESH
f32 = jnp.float32
bf16 = jnp.bfloat16

SLABS = 4
BLOCKS = 4
ROWS = 32
CHUNKS = 4
ORDER = (0, 3, 1, 2)
PLACE = (4, 4, 2, 2, 4, 4, 3, 3)
MAIN = CHUNKS * 16 + 2
EDGE = CHUNKS * 8 + 1
CROSS = CHUNKS * 2 + 1
CORNER = CHUNKS + 1


def raw_weights(element, offset, node):
    return jnp.where(element == node, 1.0 - offset, 0.0) + jnp.where(
        element + 1 == node, offset, 0.0
    )


def split(x):
    high = x.astype(bf16)
    low = (x - high.astype(f32)).astype(bf16)
    return high, low


def dot(a, b):
    return jnp.dot(a, b, preferred_element_type=f32)


def iota(shape, dim):
    return lax.broadcasted_iota(jnp.int32, shape, dim)


def spread(element, offset, pick):
    cells = element.shape[1]
    first = offset.astype(bf16).astype(f32)
    second = (offset - first).astype(bf16).astype(f32)
    third = offset - first - second
    row = iota((16, cells), 0)
    stack = jnp.where(
        row == 0,
        element.astype(f32),
        jnp.where(row == 1, first, jnp.where(row == 2, second, jnp.where(row == 3, third, 0.0))),
    )
    out = dot(stack.astype(bf16), pick)
    return out[0:1], out[1:2] + out[2:3] + out[3:4]


def kernel(
    cal, act, ef, of, es, os_, et, ot, trop, tens, unb, rel,
    out_bound, out_active,
    x_buf, ef_v, of_v, es_v, os_v, et_v, ot_v, trop_v, tens_v, unb_v, rel_v,
    w1, w2h, w2l, y_buf, tail, extra_buf,
    s_main, s_x, s_edge, s_corner,
    r_main, r_x, r_edge, r_corner,
    sem_x, sem_small,
    ss_main, ss_x, ss_edge, ss_corner,
    rs_main, rs_x, rs_edge, rs_corner, x_ready,
):
    gx, gy, gz = lax.axis_index("gx"), lax.axis_index("gy"), lax.axis_index("gz")
    last_x = lax.axis_size("gx") - 1
    blocks = ORDER

    smalls = [
        pltpu.make_async_copy(src, dst, sem_small.at[n])
        for n, (src, dst) in enumerate(
            [(ef, ef_v), (of, of_v), (et, et_v), (ot, ot_v), (es, es_v), (os_, os_v),
             (trop, trop_v), (tens, tens_v), (unb, unb_v), (rel, rel_v)]
        )
    ]
    barrier = pltpu.get_barrier_semaphore()

    def ready(x, y, z):
        pl.semaphore_signal(
            barrier, inc=1, device_id={"gx": x, "gy": y, "gz": z}, device_id_type=MESH
        )

    from_below = jnp.logical_and(gz == 0, gy > 0)
    has_edge = jnp.logical_or(from_below, gz == SLABS - 1)
    has_x = gx > 0
    sends_x = gx < last_x
    sends_edge = gz < SLABS - 1

    near = gz < 2
    relays = jnp.logical_and(gz >= 2, sends_x)

    for c in range(4):
        @pl.when(jnp.logical_and(has_x, near))
        def _():
            ready(gx - 1, c, gy)

        @pl.when(jnp.logical_and(has_x, from_below))
        def _():
            ready(gx - 1, c, gy - 1)

    @pl.when(jnp.logical_and(has_x, gz >= 2))
    def _():
        ready(gx - 1, gy, gz)

    for q in (2, 3):
        @pl.when(jnp.logical_and(sends_x, jnp.logical_not(jnp.logical_and(gy == gz, gz == q))))
        def _():
            ready(gx, gz, q)

    for copy in smalls[:6]:
        copy.start()

    @pl.when(jnp.logical_or(gy != gz, gy != 0))
    def _():
        ready(gx, 0, gy)

    loads = {}
    for j in range(BLOCKS):
        first_cell = blocks[j] * 8
        for u in range(CHUNKS):
            src = (cal, act)[u // 2].at[pl.ds(4 * (u % 2), 4), :, pl.ds(first_cell, 8), :]
            loads[j, u] = pltpu.make_async_copy(src, x_buf.at[j, u], sem_x.at[j, u])

    def issue(j):
        for u in range(CHUNKS):
            loads[j, u].start()

    issue(0)
    for copy in smalls[6:]:
        copy.start()

    def main_self(c):
        return jnp.logical_and(gy == gz, gy == c)

    def below_self(c):
        return jnp.logical_and(jnp.logical_and(gy == 1, gz == 0), gy == c)

    last_self = jnp.logical_and(gy == SLABS - 1, gz == SLABS - 1)

    for c in range(4):
        if c > 0:
            @pl.when(jnp.logical_not(main_self(c)))
            def _():
                ready(gx, c, gy)

        @pl.when(jnp.logical_and(from_below, jnp.logical_not(below_self(c))))
        def _():
            ready(gx, c, gy - 1)

    issue(1)
    edge_self = jnp.logical_and(gz == 0, gy == 1)
    expected = (
        jnp.where(gy == gz, 3, 4)
        + jnp.where(sends_x, 2, 0)
        + jnp.where(relays, jnp.where(gy == gz, 4, 5), 0)
        + jnp.where(jnp.logical_and(sends_edge, jnp.logical_not(edge_self)), 1, 0)
        + jnp.where(jnp.logical_and(sends_edge, sends_x), 1, 0)
    )

    @pl.when(jnp.logical_not(has_x))
    def _():
        r_x[...] = jnp.zeros_like(r_x)

    @pl.when(jnp.logical_not(has_edge))
    def _():
        r_edge[...] = jnp.zeros_like(r_edge)

    @pl.when(jnp.logical_not(jnp.logical_and(has_x, has_edge)))
    def _():
        r_corner[...] = jnp.zeros_like(r_corner)

    row = iota((ROWS, 1), 0)
    a_of = jnp.where(row < 24, lax.rem(row, 8), 8)
    b_of = jnp.where(row < 24, row // 8, row - 24)
    valid = row < 27
    pick_first = jnp.where(iota((256, 256), 0) == 32 * gx + iota((256, 256), 1) // 8, 1.0, 0.0).astype(bf16)
    pick_cell = iota((128, 256), 0) - lax.rem(iota((128, 256), 1), 8)
    for n in range(4):
        smalls[n].wait()
    issue(2)
    e_first = jnp.concatenate([ef_v[0:1, :], ef_v[1:2, :]], axis=1)
    o_first = jnp.concatenate([of_v[0:1, :], of_v[1:2, :]], axis=1)
    node_first = 8 * gx + a_of
    sum_first = jnp.sum(raw_weights(e_first, o_first, node_first), axis=1, keepdims=True)
    ex, ox = spread(e_first, o_first, pick_first)
    wide_first = raw_weights(ex, ox, node_first.astype(f32))
    e_third, o_third = et_v[...], ot_v[...]
    for j in range(BLOCKS):
        node_third = 8 * gz + 2 * blocks[j] + b_of
        sum_third = jnp.sum(raw_weights(e_third, o_third, node_third), axis=1, keepdims=True)
        pick = jnp.where(pick_cell == 32 * gz + 8 * blocks[j], 1.0, 0.0).astype(bf16)
        ex, ox = spread(e_third, o_third, pick)
        scale = jnp.where(valid, 1.0 / jnp.where(valid, sum_first * sum_third, 1.0), 0.0)
        wide = wide_first * raw_weights(ex, ox, node_third.astype(f32)) * scale
        high, low = split(wide)
        w1[j, 0:ROWS] = high
        w1[j, ROWS:] = low

    issue(3)
    smalls[4].wait()
    smalls[5].wait()

    def second_weights():
        node_row = iota((40, 1), 0)
        node_second = 32 * gy + node_row
        inside = jnp.logical_and(node_row < 33, node_second < 128)
        total = jnp.zeros((40, 1), f32)
        for n in range(4):
            total += jnp.sum(
                raw_weights(es_v[n : n + 1, :], os_v[n : n + 1, :], node_second), axis=1, keepdims=True
            )
        own = raw_weights(es_v[pl.ds(gy, 1), :], os_v[pl.ds(gy, 1), :], node_second)
        own = jnp.where(inside, own / jnp.where(inside, total, 1.0), 0.0)
        lane_w = iota((128, 128), 1)
        turned = jnp.transpose(jnp.concatenate([own[0:32]] * 4, axis=0))
        turned_edge = jnp.transpose(jnp.broadcast_to(own[32:33], (128, 128)))
        for k in range(4):
            group = lax.rem(gy + k, 4)
            edge_group = lax.rem(gy + 1 + k, 4)
            wide = jnp.concatenate(
                [
                    jnp.where(lane_w // 32 == group, turned, 0.0),
                    jnp.where(lane_w // 32 == edge_group, turned_edge, 0.0),
                ],
                axis=1,
            )
            high, low = split(wide)
            w2h[128 * k : 128 * (k + 1), :] = high
            w2l[128 * k : 128 * (k + 1), :] = low

    def remote(src, dst, send_sem, recv_sem, x, y, z):
        rows = {72: MAIN, 40: EDGE, 16: CROSS, 8: CORNER}[src.shape[0]]
        return pltpu.make_async_remote_copy(
            src_ref=src.at[pl.ds(0, rows)], dst_ref=dst.at[pl.ds(0, rows)], send_sem=send_sem, recv_sem=recv_sem,
            device_id={"gx": x, "gy": y, "gz": z}, device_id_type=MESH,
        )

    sub8 = iota((8, 128), 0)

    def first_stage(j, f):
        slot = (2 * j + f) % 2
        for n in range(2):
            u = 2 * f + n
            for pair in range(2):
                x = jnp.concatenate(
                    [x_buf[j, u, 2 * pair + m].reshape(256, 128) for m in range(2)], axis=1
                )
                high, low = split(x)
                twice = dot(w1[j], high)
                y = twice[0:ROWS] + twice[ROWS:] + dot(w1[j, 0:ROWS], low)
                high, low = split(y)
                columns = slice(256 * pair, 256 * (pair + 1))
                y_buf[slot, ROWS * n : ROWS * (n + 1), columns] = high
                y_buf[slot, ROWS * (2 + n) : ROWS * (3 + n), columns] = low

    sub_wide = iota((8, 256), 0)
    within = lax.rem(iota((8, 128), 1), 32)

    def chosen(where, value):
        return jnp.where(where, value[:, 128:256], 0.0)

    def finish(j, u, rows):
        parts = [rows[8 * n : 8 * (n + 1)] for n in range(4)]
        if blocks[j] in (1, 2):
            corner = pltpu.roll(tail[u, 8:16, :], 6, axis=0)
            parts[0] += tail[u, 0:8, :]
            parts[3] += jnp.where(sub_wide == 0, corner, 0.0)
        if blocks[j] in (0, 1):
            tail[u, 0:8, :] = parts[2]
            tail[u, 8:16, :] = parts[3]
        s_main[j, 16 * u : 16 * u + 8, :] = parts[0][:, 0:128]
        s_main[j, 16 * u + 8 : 16 * u + 16, :] = parts[1][:, 0:128]
        s_x[j, 2 * u : 2 * (u + 1), :] = parts[3][0:2, 0:128]
        if blocks[j] in (2, 3):
            slot = 3 - blocks[j]
            s_edge[slot, 8 * u : 8 * (u + 1), :] = parts[2][:, 0:128]
            s_corner[slot, u : u + 1, :] = parts[3][2:3, 0:128]
        first = 16 * (u % 2)
        main = chosen(within == first + 15 - sub8, parts[0]) + chosen(within == first + 7 - sub8, parts[1])
        cross = chosen(jnp.logical_and(sub8 < 2, within == 7 - 2 * u - sub8), parts[3])
        edge = chosen(within == 8 * u + 7 - sub8, parts[2])
        corner = chosen(jnp.logical_and(sub8 == 2, within == u), parts[3])
        return main, cross, edge, corner

    def second_stage(j, f):
        y = y_buf[(2 * j + f) % 2]
        twice = dot(y, w2h[...])
        n = 2 * ROWS
        z = twice[0:n] + twice[n:] + dot(y[0:n], w2l[...])
        sums = [
            a + b
            for a, b in zip(finish(j, 2 * f, z[0:ROWS]), finish(j, 2 * f + 1, z[ROWS:]))
        ]

        def row_of(value):
            return jnp.sum(value, axis=0, keepdims=True)

        s_main[j, 16 * CHUNKS + f : 16 * CHUNKS + f + 1, :] = row_of(sums[0])
        if f == 0:
            for n in range(3):
                extra_buf[8 * n : 8 * (n + 1), :] = sums[n + 1]
        else:
            rest = [row_of(sums[n + 1] + extra_buf[8 * n : 8 * (n + 1), :]) for n in range(3)]
            s_x[j, CROSS - 1 : CROSS, :] = rest[0]
            if blocks[j] in (2, 3):
                slot = 3 - blocks[j]
                s_edge[slot, EDGE - 1 : EDGE, :] = rest[1]
                s_corner[slot, CORNER - 1 : CORNER, :] = rest[2]

    both = jnp.logical_and
    copies = {}
    for j, block in enumerate(blocks):
        copies["x", j] = (sends_x, remote(
            s_x.at[j], r_x.at[gy], ss_x.at[j], rs_x.at[gy], gx + 1, gz, block))
        if block == BLOCKS - 1:
            copies["corner", 0] = (both(sends_edge, sends_x), remote(
                s_corner.at[0], r_corner.at[gy], ss_corner.at[0], rs_corner.at[gy],
                gx + 1, gz + 1, 0))
            copies["edge", 0] = (both(sends_edge, jnp.logical_not(edge_self)), remote(
                s_edge.at[0], r_edge.at[gy], ss_edge.at[0], rs_edge.at[gy], gx, gz + 1, 0))
        copies["main", j] = (jnp.logical_not(both(gy == gz, gz == block)), remote(
            s_main.at[j], r_main.at[gy], ss_main.at[j], rs_main.at[gy], gx, gz, block))
        if j == BLOCKS - 1:
            copies["corner", 1] = (sends_x, remote(
                s_corner.at[1], r_corner.at[gy], ss_corner.at[1], rs_corner.at[gy],
                gx + 1, gz, BLOCKS - 1))
            copies["edge", 1] = (jnp.logical_not(last_self), remote(
                s_edge.at[1], r_edge.at[gy], ss_edge.at[1], rs_edge.at[gy],
                gx, gz, BLOCKS - 1))

    READY = [
        [("x", 0), ("main", 0)],
        [("corner", 0), ("edge", 0), ("main", 1)],
        [("x", 2), ("main", 2)],
        [("main", 3), ("edge", 1)],
    ]
    RANK = {name: n for n, name in enumerate((
        ("x", 0), ("corner", 0), ("main", 0), ("edge", 0), ("main", 1),
        ("x", 2), ("main", 2), ("main", 3), ("edge", 1)))}

    def send(names, when=None):
        for name in names:
            condition, copy = copies[name]
            condition = condition if when is None else both(condition, when)

            @pl.when(condition)
            def _():
                copy.start()

    def enter(when):
        @pl.when(when)
        def _():
            pl.semaphore_wait(barrier, expected)

        for c in range(4):
            @pl.when(both(both(when, relays), jnp.logical_not(main_self(c))))
            def _():
                pl.semaphore_signal(
                    x_ready.at[lax.max(gz - 2, 0)], inc=1,
                    device_id={"gx": gx, "gy": c, "gz": gy}, device_id_type=MESH,
                )

        @pl.when(both(both(when, relays), gy == gz))
        def _():
            pl.semaphore_signal(x_ready.at[lax.max(gz - 2, 0)], inc=1)

    def by_gz(values):
        out = values[3]
        for n in range(3):
            out = jnp.where(gz == n, values[n], out)
        return out

    place = jnp.where(gx == 3, by_gz(PLACE[4:]), by_gz(PLACE[:4]))
    for h in range(2 * BLOCKS + 1):
        j, f = h // 2, h % 2
        if h < 2 * BLOCKS:
            for u in range(2 * f, 2 * f + 2):
                loads[j, u].wait()
        if h == 0:
            second_weights()
        else:
            second_stage((h - 1) // 2, (h - 1) % 2)
        if h < 2 * BLOCKS:
            first_stage(j, f)
        if h in PLACE:
            here = place == h
            enter(here)
            names = [name for i in range(j) for name in READY[i]]
            send(sorted(names, key=lambda name: RANK[name]), here)
        if h > min(PLACE) and f == 0:
            send(READY[j - 1], place < h)

    for n, names in ((1, [("x", 1), ("corner", 1)]), (0, [("x", 3)])):
        @pl.when(sends_x)
        def _():
            pl.semaphore_wait(x_ready.at[n], 1)

        send(names)

    for j, block in enumerate(blocks):
        @pl.when(both(gy == gz, gz == block))
        def _():
            r_main[pl.ds(gy, 1)] = s_main[j : j + 1]

    @pl.when(both(sends_edge, edge_self))
    def _():
        r_edge[pl.ds(gy, 1)] = s_edge[0:1]

    @pl.when(last_self)
    def _():
        r_edge[pl.ds(gy, 1)] = s_edge[1:2]

    def arrive(when, buf, sems, c, source):
        @pl.when(when)
        def _():
            remote(source, buf.at[c], ss_main.at[0], sems.at[c], gx, gy, gz).wait_recv()

    for n in range(6, 10):
        smalls[n].wait()
    for when, copy in copies.values():
        @pl.when(when)
        def _():
            copy.wait_send()

    for c in range(4):
        arrive(jnp.logical_not(main_self(c)), r_main, rs_main, c, s_main.at[0])
    for c in range(4):
        arrive(
            both(has_edge, jnp.logical_not(jnp.logical_or(below_self(c), both(last_self, gy == c)))),
            r_edge, rs_edge, c, s_edge.at[0],
        )
    for c in range(4):
        arrive(both(has_x, has_edge), r_corner, rs_corner, c, s_corner.at[0])
    for c in range(4):
        arrive(has_x, r_x, rs_x, c, s_x.at[0])

    top = sub8 == 0
    lane = iota((8, 128), 1)
    group = lane // 32
    lead = lax.rem(lane, 32) == 0

    def gathered(c, u):
        low_rows = (
            r_main[c, 16 * u : 16 * u + 8, :]
            + r_edge[c, 8 * u : 8 * u + 8, :]
            + jnp.where(top, r_x[c, 2 * u : 2 * u + 1, :] + r_corner[c, u : u + 1, :], 0.0)
        )
        high_rows = r_main[c, 16 * u + 8 : 16 * u + 16, :] + jnp.where(
            top, r_x[c, 2 * u + 1 : 2 * u + 2, :], 0.0
        )
        return low_rows, high_rows

    def unpicked(row, shift):
        return pltpu.roll(
            jnp.broadcast_to(row, (8, 128)), shift % 128, axis=1, stride=1, stride_axis=0
        )

    crosses = [unpicked(r_x[c, CROSS - 1 : CROSS, :], 121) for c in range(4)]

    def edges_of(c, u):
        row = 16 * CHUNKS + u // 2
        row = r_main[c, row : row + 1, :]
        corner = r_corner[c, CORNER - 1 : CORNER, :]
        corner = pltpu.roll(corner, 128 - u, axis=1) if u else corner
        cross = crosses[c]
        low_rows = (
            unpicked(row, 113 - 16 * (u % 2))
            + unpicked(r_edge[c, EDGE - 1 : EDGE, :], 121 - 8 * u)
            + jnp.where(top, cross[2 * u : 2 * u + 1] + corner, 0.0)
        )
        high_rows = unpicked(row, 121 - 16 * (u % 2)) + jnp.where(
            top, cross[2 * u + 1 : 2 * u + 2], 0.0
        )
        return low_rows, high_rows

    def by_group(values, shift):
        out = values[(0 - shift) % 4]
        for h in range(1, 4):
            out = jnp.where(group == h, values[(h - shift) % 4], out)
        return out

    drive = {}
    for u in range(CHUNKS):
        mains = [gathered(c, u) for c in range(4)]
        picked = [edges_of(c, u) for c in range(4)]
        for b in range(2):
            edges = [jnp.where(lead, picked[c][b], 0.0) for c in range(4)]
            for k in range(4):
                value = by_group([mains[c][b] for c in range(4)], k) + by_group(edges, k + 1)
                if k:
                    value = pltpu.roll(value, 128 - 32 * k, axis=1)
                drive[u // 2, 4 * (u % 2) + k, b] = value

    for b in range(2):
        bound, active = trop_v[:, b, :], tens_v[:, b, :]
        unbind, relax = unb_v[:, b, :], rel_v[:, b, :]
        keep_bound = 1.0 - step_size * unbind
        keep_active = 1.0 - step_size * relax
        for t in range(8):
            squared = drive[0, t, b] * drive[0, t, b]
            gain = (step_size * bind_rate) * (squared / (squared + half_square))
            pull = (step_size * peak_tension) * relax * drive[1, t, b]
            bound = bound * (keep_bound - gain) + gain
            active = active * keep_active + pull * bound
        out_bound[:, b, :] = bound
        out_active[:, b, :] = active


def write_out(bound, active, out_bound, out_active, sems):
    copies = [
        pltpu.make_async_copy(bound, out_bound, sems.at[0]),
        pltpu.make_async_copy(active, out_active, sems.at[1]),
    ]
    for copy in copies:
        copy.start()
    for copy in copies:
        copy.wait()


def per_device(
    calcium, activation,
    element_first, offset_first, element_second, offset_second, element_third, offset_third,
    troponin, tension, unbind_rate, relax_rate,
):
    anywhere = pl.BlockSpec(memory_space=pltpu.HBM)
    vmem = pl.BlockSpec(memory_space=pltpu.VMEM)
    dma = pltpu.SemaphoreType.DMA
    small = jax.ShapeDtypeStruct(troponin.shape, f32)
    kept = pltpu.VMEM(troponin.shape, f32)
    bound, active = pl.pallas_call(
        kernel,
        out_shape=(kept, kept),
        in_specs=[anywhere] * 12,
        out_specs=(vmem, vmem),
        scratch_shapes=[
            pltpu.VMEM((BLOCKS, CHUNKS, 4, 32, 8, 128), f32),
            pltpu.VMEM((2, 128), jnp.int32),
            pltpu.VMEM((2, 128), f32),
            pltpu.VMEM((4, 128), jnp.int32),
            pltpu.VMEM((4, 128), f32),
            pltpu.VMEM((1, 128), jnp.int32),
            pltpu.VMEM((1, 128), f32),
            *[pltpu.VMEM(troponin.shape, f32) for _ in range(4)],
            pltpu.VMEM((BLOCKS, 2 * ROWS, 256), bf16),
            pltpu.VMEM((512, 256), bf16),
            pltpu.VMEM((512, 256), bf16),
            pltpu.VMEM((2, 4 * ROWS, 512), bf16),
            pltpu.VMEM((CHUNKS, 16, 256), f32),
            pltpu.VMEM((24, 128), f32),
            pltpu.VMEM((BLOCKS, 72, 128), f32),
            pltpu.VMEM((BLOCKS, 16, 128), f32),
            pltpu.VMEM((2, 40, 128), f32),
            pltpu.VMEM((2, 8, 128), f32),
            pltpu.VMEM((4, 72, 128), f32),
            pltpu.VMEM((4, 16, 128), f32),
            pltpu.VMEM((4, 40, 128), f32),
            pltpu.VMEM((4, 8, 128), f32),
            dma((BLOCKS, CHUNKS)),
            dma((10,)),
            dma((BLOCKS,)),
            dma((BLOCKS,)),
            dma((2,)),
            dma((2,)),
            dma((4,)),
            dma((4,)),
            dma((4,)),
            dma((4,)),
            pltpu.SemaphoreType.REGULAR((2,)),
        ],
        compiler_params=pltpu.CompilerParams(
            collective_id=0, has_side_effects=True, vmem_limit_bytes=60 * 1024 * 1024
        ),
        name="restrict_and_step",
    )(
        calcium, activation,
        element_first.reshape(2, 128), offset_first.reshape(2, 128),
        element_second.reshape(4, 128), offset_second.reshape(4, 128),
        element_third.reshape(1, 128), offset_third.reshape(1, 128),
        troponin, tension, unbind_rate, relax_rate,
    )
    return pl.pallas_call(
        write_out,
        out_shape=(small, small),
        in_specs=[vmem, vmem],
        out_specs=(anywhere, anywhere),
        scratch_shapes=[dma((2,))],
        compiler_params=pltpu.CompilerParams(vmem_limit_bytes=2**20),
        name="write_out",
    )(bound, active)


def solution(mesh):
    nodes = P("gx", ("gy", "gz"), None)
    fine = P(None, "gx", "gz", "gy")
    return jax.shard_map(
        per_device,
        mesh=mesh,
        in_specs=(fine, fine, P(), P(), P(), P(), P(), P(), nodes, nodes, nodes, nodes),
        out_specs=(nodes, nodes),
        check_vma=False,
    )
```
